256 devices in a mesh: dp: 32 (over z, x_lo, core), tp: 8 (over y, x_hi).
Axes of the slice: x: 4 (x_hi: 2, x_lo: 2; x = x_hi * 2 + x_lo), y: 4, z: 8, core: 2. Of those that a mesh axis runs over, the one named last changes fastest.
Arguments:
- gate_pre: bfloat16 [24576, 7168], P('dp', 'tp'), may hold values from -6 to 6
- up_pre: bfloat16 [24576, 7168], P('dp', 'tp'), may hold values from -6 to 6
- target: bfloat16 [24576, 2048], P('dp', 'tp'), may hold values from -6 to 6
- norm_gain: float32 [2048], P('tp'), may hold values from 0.5 to 1.5
- weight: bfloat16 [32, 7168, 2048], P('dp', 'tp'), may hold values from -6 to 6
- round_index: int32 [1], replicated, may hold values from 0 to 9999
Outputs:
- normed: bfloat16 [24576, 2048], P('dp', 'tp')
- mixed: bfloat16 [32, 7168, 2048], P('dp', 'tp')
The draws below stay inside these ranges and needn't reach their ends.
All inputs are finite; a program needn't handle non-finite values.
Results may differ from the reference program's by a relative error of at most 0.001.
The reference program's roundings to bfloat16 on the way (of `hidden`, `grad_out` and `updated`) count: a program that leaves them out, or rounds other values in their place, can miss the bound.
Values may be sent and summed in bfloat16 or wider, within the bound.
A program may use at most 64 MiB of HBM per device.

```python
import math
import jax
import jax.numpy as jnp
from jax import lax

D = 2048
FF = 7168
TOK = 768
TOKENS = 24576
N_DP = 32


def block_scale(key, dims, pieces, smallest, high):
    factor_of, own = 1.0, jax.random.fold_in(key, 6)
    for dim, shards_of in pieces:
        steps = jnp.exp(jax.random.uniform(jax.random.fold_in(own, dim), (shards_of,), jnp.float32, smallest / len(pieces), high / len(pieces)))
        factor_of = factor_of * jnp.repeat(steps, dims[dim] // shards_of).reshape([-1 if axis == dim else 1 for axis in range(len(dims))])
    return factor_of


def centred(key, extent, scale, reach, split=(), kind=jnp.bfloat16):
    drawn = jax.random.normal(key, extent, jnp.float32) * scale
    if len(split) > 0:
        drawn = block_scale(key, extent, split, -0.22, 0.18) * drawn
    return jnp.clip(drawn, min=-reach, max=reach).astype(kind)


def setup_inputs(seed: int = 0) -> dict:
    arg_keys = jax.random.split(jax.random.key(seed), 7)
    gate_pre = centred(arg_keys[0], (TOKENS, FF), 1.0, 6.0, ((0, 32), (1, 8)))
    up_pre = centred(arg_keys[1], (TOKENS, FF), 1.0, 6.0, ((0, 32), (1, 8)))
    target = centred(arg_keys[2], (TOKENS, D), 1.0, 6.0, ((0, 32), (1, 8)))
    norm_gain = jnp.clip(1.0 + 0.1 * jax.random.normal(arg_keys[3], (D,), jnp.float32), 0.5, 1.5)
    weight = centred(arg_keys[4], (N_DP, FF, D), 1.0, 6.0, ((0, 32), (1, 8)))
    round_index = jax.random.randint(arg_keys[5], (1,), 0, 10000).astype(jnp.int32)
    return {"gate_pre": gate_pre, "up_pre": up_pre, "target": target, "norm_gain": norm_gain, "weight": weight, "round_index": round_index}


EPSILON = 1e-06

def step_rate(round_index):
    phase = (round_index[0] % 1000).astype(jnp.float32) * jnp.float32(2.0 * math.pi / 1000.0)
    return jnp.float32(0.25) * (jnp.float32(0.55) + jnp.float32(0.45) * jnp.cos(phase))

def replica_step(inputs, norm_gain, rate):
    gate_rows, up_rows, target_rows, weight_rows = inputs
    out_scale = FF ** (-0.5)
    hidden = (jax.nn.silu(gate_rows.astype(jnp.float32)) * up_rows.astype(jnp.float32)).astype(jnp.bfloat16)
    summed = jnp.dot(hidden, weight_rows, preferred_element_type=jnp.float32) * out_scale
    inv_rms = lax.rsqrt(lax.optimization_barrier(jnp.mean(summed * summed, axis=1, keepdims=True)) + EPSILON)
    normal = summed * inv_rms
    output = normal * norm_gain
    grad_norm = (output - target_rows.astype(jnp.float32)) * norm_gain
    inner = lax.optimization_barrier(jnp.mean(grad_norm * normal, axis=1, keepdims=True))
    grad_out = (inv_rms * (grad_norm - normal * inner)).astype(jnp.bfloat16)
    weight_grad = lax.dot_general(hidden, grad_out, (((0,), (0,)), ((), ())), preferred_element_type=jnp.float32) * out_scale
    updated = (weight_rows.astype(jnp.float32) - rate * weight_grad).astype(jnp.bfloat16)
    return (output.astype(jnp.bfloat16), updated)

def reference(gate_pre, up_pre, target, norm_gain, weight, round_index):
    gate_blocks = gate_pre.reshape(N_DP, TOK, FF)
    up_blocks = up_pre.reshape(N_DP, TOK, FF)
    target_blocks = target.reshape(N_DP, TOK, D)
    rate = step_rate(round_index)

    def one_replica(inputs):
        return replica_step(inputs, norm_gain, rate)
    normed, updated = lax.map(one_replica, (gate_blocks, up_blocks, target_blocks, weight))
    levels = N_DP.bit_length() - 1
    offset = jnp.left_shift(jnp.int32(1), (round_index[0] % levels).astype(jnp.int32))
    source = ((jnp.arange(N_DP, dtype=jnp.int32) - offset) % N_DP).astype(jnp.int32)
    peer_rows = updated[source]
    mixed = (0.5 * (updated.astype(jnp.float32) + peer_rows.astype(jnp.float32))).astype(jnp.bfloat16)
    return (normed.reshape(N_DP * TOK, D), mixed)
```

```python
import functools
import math

import jax
import jax.numpy as jnp
from jax import lax
from jax.experimental import pallas as pl
from jax.experimental.pallas import tpu as pltpu
from jax.sharding import Mesh
from jax.sharding import PartitionSpec as P

FF = 7168
EPSILON = 1e-06
CODE_MAX = 32767.0
N_CHUNKS = 3
N_TP = 8
N_Y = 4
MESH = pl.DeviceIdType.MESH
ROWS = 64


def step_rate(round_index):
    phase = (round_index[0] % 1000).astype(jnp.float32) * jnp.float32(2.0 * math.pi / 1000.0)
    return jnp.float32(0.25) * (jnp.float32(0.55) + jnp.float32(0.45) * jnp.cos(phase))


def across(rows, lanes=128):
    n = rows.shape[1]
    return jnp.broadcast_to(rows[None], (lanes // 8, 8, n)).reshape(lanes, n).T


def kernel(
    level, nz,
    gate, up, target, gain, weight, rate,
    normed, mixed,
    gate_v, up_v, target_v, w_v, h_v, ht_v, p_v, mx_v, own_v, q_v, qs_v, rq_v, rs_v, tr_v, st_v, rst_v,
    norm_v, grad_v, upd_v, peer_v,
    in_sem, w_sem, out_sem, mix_sem, qss, qrs, sss, srs, tss, trs, bss, brs, css, crs,
):
    share = target_v.shape[1]
    ff = w_v.shape[1]
    chunk = h_v.shape[1]
    z, xl, c, y, xh = (lax.axis_index(a) for a in ("z", "xl", "c", "y", "xh"))
    mine = y * 2 + xh

    def offset(k):
        j = lax.div(k, 2)
        return lax.rem(lax.div(j * (j + 1), 2), 4), lax.rem(k, 2)

    def member(k):
        dy, dx = offset(k)
        return lax.rem(y + dy, N_Y), lax.rem(xh + dx, 2)

    def device(k):
        py, px = member(k)
        return {"y": py, "xh": px}

    def owner(k):
        py, px = member(k)
        return py * 2 + px

    def seen_as(k):
        j = lax.div(k, 2)
        return (2 * j - 3 * lax.div(j, 2)) * 2 + lax.rem(k, 2)

    def gossip(by):
        to = lax.rem(z * 4 + xl * 2 + c + by, nz * 4)
        return {"z": lax.div(to, 4), "xl": lax.rem(lax.div(to, 2), 2), "c": lax.rem(to, 2)}

    target_device = gossip(1 << level)
    source_device = gossip(nz * 4 - (1 << level))

    def load(i, which):
        src, dst = ((gate, gate_v), (up, up_v))[which]
        return pltpu.make_async_copy(src.at[pl.ds(i * chunk, chunk)], dst.at[i], in_sem.at[which, i])

    def load_w(k):
        return pltpu.make_async_copy(weight.at[:, pl.ds(k * share, share)], w_v.at[k], w_sem.at[k])

    target_load = pltpu.make_async_copy(target, target_v, in_sem.at[2, 0])
    for which in range(2):
        load(0, which).start()
    for k in range(N_TP):
        load_w(k).start()
    for i in range(1, N_CHUNKS):
        for which in range(2):
            load(i, which).start()
    target_load.start()

    barrier = pltpu.get_barrier_semaphore()
    for k in range(1, N_TP):
        pl.semaphore_signal(barrier, inc=1, device_id=device(jnp.int32(k)), device_id_type=MESH)
    pl.semaphore_signal(barrier, inc=1, device_id=source_device, device_id_type=MESH)

    def code_copy(i, k):
        s = seen_as(k)
        return pltpu.make_async_remote_copy(
            src_ref=q_v.at[i, k], dst_ref=rq_v.at[i, s], send_sem=qss.at[i, k], recv_sem=qrs.at[i, s],
            device_id=device(k), device_id_type=MESH,
        )

    def scale_copy(i, k):
        s = seen_as(k)
        return pltpu.make_async_remote_copy(
            src_ref=qs_v.at[i], dst_ref=rs_v.at[i, s], send_sem=sss.at[i, k], recv_sem=srs.at[i, s],
            device_id=device(k), device_id_type=MESH,
        )

    def project(i, _):
        load(i, 0).wait()
        load(i, 1).wait()

        def hidden_rows(r, _):
            rows = pl.ds(r * ROWS, ROWS)
            v = gate_v[i, rows, :].astype(jnp.float32)
            h = v / (1.0 + jnp.exp(-v)) * up_v[i, rows, :].astype(jnp.float32)
            h_v[i, rows, :] = h.astype(jnp.bfloat16)
            return 0

        lax.fori_loop(0, chunk // ROWS, hidden_rows, 0)

        @pl.when(i == 0)
        def _():
            for k in range(N_TP):
                load_w(k).wait()

        mx_v[...] = jnp.zeros_like(mx_v)

        def product(k, _):
            part = jnp.dot(h_v[i], w_v[k], preferred_element_type=jnp.float32)
            p_v[k] = part
            size = jnp.abs(part)
            for half in range(share // 128):
                mx_v[...] = jnp.maximum(mx_v[...], size[:, half * 128 : (half + 1) * 128])
            return 0

        lax.fori_loop(0, N_TP, product, 0)
        own_v[i] = p_v[mine]
        largest = jnp.maximum(jnp.max(mx_v[...], axis=1, keepdims=True), 1e-30)
        mx_v[...] = jnp.broadcast_to(CODE_MAX / largest, mx_v.shape)
        qs_v[i] = jnp.broadcast_to(largest * (1.0 / CODE_MAX), mx_v.shape).T[0:8, :]

        @pl.when(i == 0)
        def _():
            pl.semaphore_wait(barrier, N_TP)

        def code(k, _):
            at = owner(k)

            def code_rows(r, _):
                rows = pl.ds(r * ROWS, ROWS)
                inverse = mx_v[rows, :]
                for half in range(share // 128):
                    lanes = slice(half * 128, (half + 1) * 128)
                    q = jnp.round(p_v[at, rows, lanes] * inverse)
                    q_v[i, k, rows, lanes] = q.astype(jnp.int32).astype(jnp.int16)
                return 0

            lax.fori_loop(0, chunk // ROWS, code_rows, 0)
            scale_copy(i, k).start()
            code_copy(i, k).start()
            return 0

        lax.fori_loop(1, N_TP, code, 0)
        return 0

    lax.fori_loop(0, N_CHUNKS, project, 0)

    for i in range(N_CHUNKS):
        ht_v[:, i * chunk : (i + 1) * chunk] = h_v[i].T

    def stat_copy(i, k):
        s = seen_as(k)
        return pltpu.make_async_remote_copy(
            src_ref=st_v.at[i], dst_ref=rst_v.at[i, s], send_sem=tss.at[i, k], recv_sem=trs.at[i, s],
            device_id=device(k), device_id_type=MESH,
        )

    target_load.wait()
    sub = lax.broadcasted_iota(jnp.int32, (8, chunk), 0)
    lane = lax.broadcasted_iota(jnp.int32, (ROWS, 128), 1)

    def reduce(i, _):
        scales = jnp.zeros((8, chunk), jnp.float32)
        for k in range(1, N_TP):
            scale_copy(i, jnp.int32(k)).wait_recv()
        for k in range(1, N_TP):
            scales = jnp.where(sub == k, rs_v[i, k], scales)
        tr_v[...] = across(scales)
        for k in range(1, N_TP):
            code_copy(i, jnp.int32(k)).wait_recv()

        def reduce_rows(r, _):
            rows = pl.ds(r * ROWS, ROWS)
            total = own_v[i, rows, :]
            scale = tr_v[rows, :]
            for k in range(1, N_TP):
                total = total + rq_v[i, k, rows, :].astype(jnp.int32).astype(jnp.float32) * scale[:, k : k + 1]
            s = total * FF ** (-0.5)
            own_v[i, rows, :] = s
            g = gain[...]
            t = target_v[pl.ds(i * chunk + r * ROWS, ROWS), :].astype(jnp.float32)
            gs = g * s
            a = jnp.sum(s * s, axis=1, keepdims=True)
            b = jnp.sum(gs * gs, axis=1, keepdims=True)
            d = jnp.sum(gs * t, axis=1, keepdims=True)
            tr_v[rows, :] = jnp.where(lane == 0, a, jnp.where(lane == 1, b, d))
            return 0

        lax.fori_loop(0, chunk // ROWS, reduce_rows, 0)
        st_v[i] = tr_v[...].T[0:8, :]

        def send(k, _):
            stat_copy(i, k).start()
            return 0

        lax.fori_loop(1, N_TP, send, 0)
        return 0

    lax.fori_loop(0, N_CHUNKS, reduce, 0)

    width = share * N_TP

    def finish(i, _):
        sums = st_v[i]
        for k in range(1, N_TP):
            stat_copy(i, jnp.int32(k)).wait_recv()
        for k in range(1, N_TP):
            sums = sums + rst_v[i, k]
        tr_v[...] = across(sums)

        def finish_rows(r, _):
            rows = pl.ds(r * ROWS, ROWS)
            at = pl.ds(i * chunk + r * ROWS, ROWS)
            sums = tr_v[rows, :] * (1.0 / width)
            inv = lax.rsqrt(sums[:, 0:1] + EPSILON)
            inner = inv * inv * sums[:, 1:2] - inv * sums[:, 2:3]
            g = gain[...]
            normal = own_v[i, rows, :] * inv
            output = normal * g
            grad_norm = (output - target_v[at, :].astype(jnp.float32)) * g
            norm_v[at, :] = output.astype(jnp.bfloat16)
            grad_v[mine, at, :] = (inv * (grad_norm - normal * inner)).astype(jnp.bfloat16)
            return 0

        lax.fori_loop(0, chunk // ROWS, finish_rows, 0)
        return 0

    lax.fori_loop(0, N_CHUNKS, finish, 0)

    def grad_copy(which, k):
        s = seen_as(k) if which == 0 else seen_as(k) + 1
        at = owner(jnp.int32(which))
        return pltpu.make_async_remote_copy(
            src_ref=grad_v.at[at], dst_ref=grad_v.at[at], send_sem=bss.at[k + which], recv_sem=brs.at[s],
            device_id=device(k), device_id_type=MESH,
        )

    def grad_arrival(k):
        at = owner(k)
        return pltpu.make_async_remote_copy(
            src_ref=grad_v.at[at], dst_ref=grad_v.at[at], send_sem=bss.at[k], recv_sem=brs.at[k],
            device_id=device(k), device_id_type=MESH,
        )

    for k in (1, 2, 4, 6):
        grad_copy(0, jnp.int32(k)).start()
    normed_out = pltpu.make_async_copy(norm_v, normed, out_sem.at[0])
    normed_out.start()

    def gossip_copy(k):
        at = owner(k)
        return pltpu.make_async_remote_copy(
            src_ref=upd_v.at[at], dst_ref=peer_v.at[at], send_sem=css.at[k], recv_sem=crs.at[k],
            device_id=target_device, device_id_type=MESH,
        )

    step = rate[0]

    def update(k, _):
        at = owner(k)

        @pl.when(k > 0)
        def _():
            grad_arrival(k).wait_recv()

        @pl.when(k == 1)
        def _():
            for j in (2, 4, 6):
                grad_copy(1, jnp.int32(j)).start()

        weight_grad = jnp.dot(ht_v[...], grad_v[at], preferred_element_type=jnp.float32) * FF ** (-0.5)
        upd_v[at] = (w_v[at].astype(jnp.float32) - step * weight_grad).astype(jnp.bfloat16)
        gossip_copy(k).start()
        return 0

    lax.fori_loop(0, N_TP, update, 0)

    def mixed_out(k):
        at = owner(k)
        return pltpu.make_async_copy(
            w_v.at[at], mixed.at[:, pl.ds(pl.multiple_of(at * share, share), share)], mix_sem.at[k]
        )

    def average(k, _):
        at = owner(k)
        gossip_copy(k).wait_recv()

        def average_rows(r, _):
            rows = pl.ds(r * ROWS, ROWS)
            both = upd_v[at, rows, :].astype(jnp.float32) + peer_v[at, rows, :].astype(jnp.float32)
            w_v[at, rows, :] = (0.5 * both).astype(jnp.bfloat16)
            return 0

        lax.fori_loop(0, ff // ROWS, average_rows, 0)
        mixed_out(k).start()
        return 0

    lax.fori_loop(0, N_TP, average, 0)

    def drain(k, _):
        def drain_chunk(i, _):
            code_copy(i, k).wait_send()
            scale_copy(i, k).wait_send()
            stat_copy(i, k).wait_send()
            return 0

        lax.fori_loop(0, N_CHUNKS, drain_chunk, 0)
        grad_arrival(k).wait_send()
        return 0

    lax.fori_loop(1, N_TP, drain, 0)

    def drain_mixed(k, _):
        gossip_copy(k).wait_send()
        mixed_out(k).wait()
        return 0

    lax.fori_loop(0, N_TP, drain_mixed, 0)
    normed_out.wait()


def step_at(level, nz, gate, up, target, gain, weight, rate):
    tok, ff = gate.shape
    share = target.shape[1]
    chunk = tok // N_CHUNKS
    bf16, f32, i16 = jnp.bfloat16, jnp.float32, jnp.int16
    dma = pltpu.SemaphoreType.DMA
    hbm = pl.BlockSpec(memory_space=pl.ANY)
    return pl.pallas_call(
        functools.partial(kernel, level, nz),
        out_shape=(
            jax.ShapeDtypeStruct((tok, share), bf16),
            jax.ShapeDtypeStruct(weight.shape, bf16),
        ),
        in_specs=[hbm, hbm, hbm, pl.BlockSpec(memory_space=pltpu.VMEM), hbm, pl.BlockSpec(memory_space=pltpu.SMEM)],
        out_specs=(hbm, hbm),
        scratch_shapes=[
            pltpu.VMEM((N_CHUNKS, chunk, ff), bf16),
            pltpu.VMEM((N_CHUNKS, chunk, ff), bf16),
            pltpu.VMEM((tok, share), bf16),
            pltpu.VMEM((N_TP, ff, share), bf16),
            pltpu.VMEM((N_CHUNKS, chunk, ff), bf16),
            pltpu.VMEM((ff, tok), bf16),
            pltpu.VMEM((N_TP, chunk, share), f32),
            pltpu.VMEM((chunk, 128), f32),
            pltpu.VMEM((N_CHUNKS, chunk, share), f32),
            pltpu.VMEM((N_CHUNKS, N_TP, chunk, share), i16),
            pltpu.VMEM((N_CHUNKS, 8, chunk), f32),
            pltpu.VMEM((N_CHUNKS, N_TP, chunk, share), i16),
            pltpu.VMEM((N_CHUNKS, N_TP, 8, chunk), f32),
            pltpu.VMEM((chunk, 128), f32),
            pltpu.VMEM((N_CHUNKS, 8, chunk), f32),
            pltpu.VMEM((N_CHUNKS, N_TP, 8, chunk), f32),
            pltpu.VMEM((tok, share), bf16),
            pltpu.VMEM((N_TP, tok, share), bf16),
            pltpu.VMEM((N_TP, ff, share), bf16),
            pltpu.VMEM((N_TP, ff, share), bf16),
            dma((3, N_CHUNKS)),
            dma((N_TP,)),
            dma((1,)),
            dma((N_TP,)),
            dma((N_CHUNKS, N_TP)),
            dma((N_CHUNKS, N_TP)),
            dma((N_CHUNKS, N_TP)),
            dma((N_CHUNKS, N_TP)),
            dma((N_CHUNKS, N_TP)),
            dma((N_CHUNKS, N_TP)),
            dma((N_TP,)),
            dma((N_TP,)),
            dma((N_TP,)),
            dma((N_TP,)),
        ],
        compiler_params=pltpu.CompilerParams(
            collective_id=level + 1, has_side_effects=True, vmem_limit_bytes=56 << 20
        ),
        name=f"step_level{level}",
    )(gate, up, target, gain, weight, rate)


def shards(nz, gate_pre, up_pre, target, norm_gain, weight, round_index):
    levels = (nz * 4).bit_length() - 1
    rate = step_rate(round_index).reshape(1)
    level = round_index[0] % levels
    operands = (gate_pre, up_pre, target, norm_gain.reshape(1, -1), weight[0], rate)
    branches = [functools.partial(step_at, number, nz) for number in range(levels)]
    normed, mixed = lax.switch(level, branches, *operands)
    return (normed, mixed[None])


def solution(mesh):
    nz = mesh.shape["dp"] // 4
    axes = ("z", "xl", "c", "y", "xh")
    finer = Mesh(mesh.devices.reshape(nz, 2, 2, N_Y, 2), axes)
    dp, tp = axes[:3], axes[3:]
    return jax.shard_map(
        functools.partial(shards, nz),
        mesh=finer,
        in_specs=(P(dp, tp), P(dp, tp), P(dp, tp), P(tp), P(dp, tp, None), P()),
        out_specs=(P(dp, tp), P(dp, tp, None)),
        check_vma=False,
    )
```

```python
import functools
import math

import jax
import jax.numpy as jnp
from jax import lax
from jax.experimental import pallas as pl
from jax.experimental.pallas import tpu as pltpu
from jax.sharding import Mesh
from jax.sharding import PartitionSpec as P

FF = 7168
EPSILON = 1e-06
CODE_MAX = 32767.0
N_CHUNKS = 3
N_TP = 8
N_Y = 4
MESH = pl.DeviceIdType.MESH
RELAYED = 2
LAG = 2
ROWS = 64


def step_rate(round_index):
    phase = (round_index[0] % 1000).astype(jnp.float32) * jnp.float32(2.0 * math.pi / 1000.0)
    return jnp.float32(0.25) * (jnp.float32(0.55) + jnp.float32(0.45) * jnp.cos(phase))


def across(rows, lanes=128):
    n = rows.shape[1]
    return jnp.broadcast_to(rows[None], (lanes // 8, 8, n)).reshape(lanes, n).T


def kernel(
    level, nz,
    gate, up, target, gain, weight, rate,
    normed, mixed,
    gate_v, up_v, target_v, w_v, h_v, ht_v, p_v, mx_v, own_v, q_v, qs_v, rq_v, rs_v, tr_v, st_v, rst_v,
    norm_v, grad_v, upd_v, peer_v, relay_v,
    in_sem, w_sem, out_sem, mix_sem, qss, qrs, sss, srs, tss, trs, bss, brs, css, crs, fss, frs,
):
    share = target_v.shape[1]
    ff = w_v.shape[1]
    chunk = h_v.shape[1]
    z, xl, c, y, xh = (lax.axis_index(a) for a in ("z", "xl", "c", "y", "xh"))
    mine = y * 2 + xh

    def offset(k):
        j = lax.div(k, 2)
        return lax.rem(lax.div(j * (j + 1), 2), 4), lax.rem(k, 2)

    def member(k):
        dy, dx = offset(k)
        return lax.rem(y + dy, N_Y), lax.rem(xh + dx, 2)

    def device(k):
        py, px = member(k)
        return {"y": py, "xh": px}

    def owner(k):
        py, px = member(k)
        return py * 2 + px

    def seen_as(k):
        j = lax.div(k, 2)
        return (2 * j - 3 * lax.div(j, 2)) * 2 + lax.rem(k, 2)

    def gossip(by):
        to = lax.rem(z * 4 + xl * 2 + c + by, nz * 4)
        return {"z": lax.div(to, 4), "xl": lax.rem(lax.div(to, 2), 2), "c": lax.rem(to, 2)}

    target_device = gossip(1 << level)
    source_device = gossip(nz * 4 - (1 << level))
    diagonal = level == 1
    around = RELAYED if level == 3 and nz == 8 else 0
    if diagonal:
        sends_far = xl == 1
        relays = xl == 0
        onward = {"z": lax.rem(z + 1, nz)}
        behind = {"z": lax.rem(z + nz - 1, nz)}
        side = {"xl": 1 - xl}
    elif around:
        onward = {"z": lax.rem(z + nz - 3, nz)}
        behind = {"z": lax.rem(z + 3, nz)}

    def load(i, which):
        src, dst = ((gate, gate_v), (up, up_v))[which]
        return pltpu.make_async_copy(src.at[pl.ds(i * chunk, chunk)], dst.at[i], in_sem.at[which, i])

    def load_w(k):
        return pltpu.make_async_copy(weight.at[:, pl.ds(k * share, share)], w_v.at[k], w_sem.at[k])

    target_load = pltpu.make_async_copy(target, target_v, in_sem.at[2, 0])
    for which in range(2):
        load(0, which).start()
    for k in range(N_TP):
        load_w(k).start()
    for i in range(1, N_CHUNKS):
        for which in range(2):
            load(i, which).start()
    target_load.start()

    barrier = pltpu.get_barrier_semaphore()
    for k in range(1, N_TP):
        pl.semaphore_signal(barrier, inc=1, device_id=device(jnp.int32(k)), device_id_type=MESH)
    if diagonal:

        pl.semaphore_signal(barrier, inc=1, device_id=side, device_id_type=MESH)

        @pl.when(relays)
        def _():
            pl.semaphore_signal(barrier, inc=1, device_id=behind, device_id_type=MESH)

    else:
        pl.semaphore_signal(barrier, inc=1, device_id=source_device, device_id_type=MESH)
        if around:
            pl.semaphore_signal(barrier, inc=1, device_id=behind, device_id_type=MESH)

    def code_copy(i, k):
        s = seen_as(k)
        return pltpu.make_async_remote_copy(
            src_ref=q_v.at[i, k], dst_ref=rq_v.at[i, s], send_sem=qss.at[i, k], recv_sem=qrs.at[i, s],
            device_id=device(k), device_id_type=MESH,
        )

    def scale_copy(i, k):
        s = seen_as(k)
        return pltpu.make_async_remote_copy(
            src_ref=qs_v.at[i], dst_ref=rs_v.at[i, s], send_sem=sss.at[i, k], recv_sem=srs.at[i, s],
            device_id=device(k), device_id_type=MESH,
        )

    def project(i, _):
        load(i, 0).wait()
        load(i, 1).wait()

        def hidden_rows(r, _):
            rows = pl.ds(r * ROWS, ROWS)
            v = gate_v[i, rows, :].astype(jnp.float32)
            h = v / (1.0 + jnp.exp(-v)) * up_v[i, rows, :].astype(jnp.float32)
            h_v[i, rows, :] = h.astype(jnp.bfloat16)
            return 0

        lax.fori_loop(0, chunk // ROWS, hidden_rows, 0)

        @pl.when(i == 0)
        def _():
            for k in range(N_TP):
                load_w(k).wait()

        mx_v[...] = jnp.zeros_like(mx_v)

        def product(k, _):
            part = jnp.dot(h_v[i], w_v[k], preferred_element_type=jnp.float32)
            p_v[k] = part
            size = jnp.abs(part)
            for half in range(share // 128):
                mx_v[...] = jnp.maximum(mx_v[...], size[:, half * 128 : (half + 1) * 128])
            return 0

        lax.fori_loop(0, N_TP, product, 0)
        own_v[i] = p_v[mine]
        largest = jnp.maximum(jnp.max(mx_v[...], axis=1, keepdims=True), 1e-30)
        mx_v[...] = jnp.broadcast_to(CODE_MAX / largest, mx_v.shape)
        qs_v[i] = jnp.broadcast_to(largest * (1.0 / CODE_MAX), mx_v.shape).T[0:8, :]

        @pl.when(i == 0)
        def _():
            pl.semaphore_wait(barrier, N_TP + (1 - xl if diagonal else 1 if around else 0))

        def code(k, _):
            at = owner(k)

            def code_rows(r, _):
                rows = pl.ds(r * ROWS, ROWS)
                inverse = mx_v[rows, :]
                for half in range(share // 128):
                    lanes = slice(half * 128, (half + 1) * 128)
                    q = jnp.round(p_v[at, rows, lanes] * inverse)
                    q_v[i, k, rows, lanes] = q.astype(jnp.int32).astype(jnp.int16)
                return 0

            lax.fori_loop(0, chunk // ROWS, code_rows, 0)
            scale_copy(i, k).start()
            code_copy(i, k).start()
            return 0

        lax.fori_loop(1, N_TP, code, 0)
        return 0

    lax.fori_loop(0, N_CHUNKS, project, 0)

    for i in range(N_CHUNKS):
        ht_v[:, i * chunk : (i + 1) * chunk] = h_v[i].T

    def stat_copy(i, k):
        s = seen_as(k)
        return pltpu.make_async_remote_copy(
            src_ref=st_v.at[i], dst_ref=rst_v.at[i, s], send_sem=tss.at[i, k], recv_sem=trs.at[i, s],
            device_id=device(k), device_id_type=MESH,
        )

    target_load.wait()
    sub = lax.broadcasted_iota(jnp.int32, (8, chunk), 0)
    lane = lax.broadcasted_iota(jnp.int32, (ROWS, 128), 1)

    def reduce(i, _):
        scales = jnp.zeros((8, chunk), jnp.float32)
        for k in range(1, N_TP):
            scale_copy(i, jnp.int32(k)).wait_recv()
        for k in range(1, N_TP):
            scales = jnp.where(sub == k, rs_v[i, k], scales)
        tr_v[...] = across(scales)
        for k in range(1, N_TP):
            code_copy(i, jnp.int32(k)).wait_recv()

        def reduce_rows(r, _):
            rows = pl.ds(r * ROWS, ROWS)
            total = own_v[i, rows, :]
            scale = tr_v[rows, :]
            for k in range(1, N_TP):
                total = total + rq_v[i, k, rows, :].astype(jnp.int32).astype(jnp.float32) * scale[:, k : k + 1]
            s = total * FF ** (-0.5)
            own_v[i, rows, :] = s
            g = gain[...]
            t = target_v[pl.ds(i * chunk + r * ROWS, ROWS), :].astype(jnp.float32)
            gs = g * s
            a = jnp.sum(s * s, axis=1, keepdims=True)
            b = jnp.sum(gs * gs, axis=1, keepdims=True)
            d = jnp.sum(gs * t, axis=1, keepdims=True)
            tr_v[rows, :] = jnp.where(lane == 0, a, jnp.where(lane == 1, b, d))
            return 0

        lax.fori_loop(0, chunk // ROWS, reduce_rows, 0)
        st_v[i] = tr_v[...].T[0:8, :]

        def send(k, _):
            stat_copy(i, k).start()
            return 0

        lax.fori_loop(1, N_TP, send, 0)
        return 0

    lax.fori_loop(0, N_CHUNKS, reduce, 0)

    width = share * N_TP

    def finish(i, _):
        sums = st_v[i]
        for k in range(1, N_TP):
            stat_copy(i, jnp.int32(k)).wait_recv()
        for k in range(1, N_TP):
            sums = sums + rst_v[i, k]
        tr_v[...] = across(sums)

        def finish_rows(r, _):
            rows = pl.ds(r * ROWS, ROWS)
            at = pl.ds(i * chunk + r * ROWS, ROWS)
            sums = tr_v[rows, :] * (1.0 / width)
            inv = lax.rsqrt(sums[:, 0:1] + EPSILON)
            inner = inv * inv * sums[:, 1:2] - inv * sums[:, 2:3]
            g = gain[...]
            normal = own_v[i, rows, :] * inv
            output = normal * g
            grad_norm = (output - target_v[at, :].astype(jnp.float32)) * g
            norm_v[at, :] = output.astype(jnp.bfloat16)
            grad_v[mine, at, :] = (inv * (grad_norm - normal * inner)).astype(jnp.bfloat16)
            return 0

        lax.fori_loop(0, chunk // ROWS, finish_rows, 0)
        return 0

    lax.fori_loop(0, N_CHUNKS, finish, 0)

    def grad_copy(which, k):
        s = seen_as(k) if which == 0 else seen_as(k) + 1
        at = owner(jnp.int32(which))
        return pltpu.make_async_remote_copy(
            src_ref=grad_v.at[at], dst_ref=grad_v.at[at], send_sem=bss.at[k + which], recv_sem=brs.at[s],
            device_id=device(k), device_id_type=MESH,
        )

    def grad_arrival(k):
        at = owner(k)
        return pltpu.make_async_remote_copy(
            src_ref=grad_v.at[at], dst_ref=grad_v.at[at], send_sem=bss.at[k], recv_sem=brs.at[k],
            device_id=device(k), device_id_type=MESH,
        )

    for k in (1, 2, 4, 6):
        grad_copy(0, jnp.int32(k)).start()
    normed_out = pltpu.make_async_copy(norm_v, normed, out_sem.at[0])
    normed_out.start()

    def gossip_copy(k):
        at = owner(k)
        return pltpu.make_async_remote_copy(
            src_ref=upd_v.at[at], dst_ref=peer_v.at[at], send_sem=css.at[k], recv_sem=crs.at[k],
            device_id=target_device, device_id_type=MESH,
        )

    def first_leg(k):
        at = owner(k)
        return pltpu.make_async_remote_copy(
            src_ref=upd_v.at[at], dst_ref=relay_v.at[k], send_sem=css.at[k], recv_sem=frs.at[k],
            device_id=side if diagonal else onward, device_id_type=MESH,
        )

    def second_leg(k):
        at = owner(k)
        return pltpu.make_async_remote_copy(
            src_ref=relay_v.at[k], dst_ref=peer_v.at[at], send_sem=fss.at[k], recv_sem=crs.at[k],
            device_id=onward, device_id_type=MESH,
        )

    def forward(k):
        first_leg(k).wait_recv()
        second_leg(k).start()

    def send_updated(k):
        if diagonal:

            @pl.when(sends_far)
            def _():
                first_leg(k).start()

            @pl.when(jnp.logical_not(sends_far))
            def _():
                gossip_copy(k).start()

            @pl.when(jnp.logical_and(relays, k >= LAG))
            def _():
                forward(k - LAG)

        elif around:

            @pl.when(k < around)
            def _():
                first_leg(k).start()

            @pl.when(k >= around)
            def _():
                gossip_copy(k).start()

        else:
            gossip_copy(k).start()

    step = rate[0]

    def update(k, _):
        at = owner(k)

        @pl.when(k > 0)
        def _():
            grad_arrival(k).wait_recv()

        @pl.when(k == 1)
        def _():
            for j in (2, 4, 6):
                grad_copy(1, jnp.int32(j)).start()

        weight_grad = jnp.dot(ht_v[...], grad_v[at], preferred_element_type=jnp.float32) * FF ** (-0.5)
        upd_v[at] = (w_v[at].astype(jnp.float32) - step * weight_grad).astype(jnp.bfloat16)
        send_updated(k)
        return 0

    lax.fori_loop(0, N_TP, update, 0)
    if diagonal:

        @pl.when(relays)
        def _():
            for k in range(N_TP - LAG, N_TP):
                forward(jnp.int32(k))

    for k in range(around):
        forward(jnp.int32(k))

    def mixed_out(k):
        at = owner(k)
        return pltpu.make_async_copy(
            w_v.at[at], mixed.at[:, pl.ds(pl.multiple_of(at * share, share), share)], mix_sem.at[k]
        )

    def average(number, _):
        k = lax.rem(number + around, N_TP)
        at = owner(k)
        gossip_copy(k).wait_recv()

        def average_rows(r, _):
            rows = pl.ds(r * ROWS, ROWS)
            both = upd_v[at, rows, :].astype(jnp.float32) + peer_v[at, rows, :].astype(jnp.float32)
            w_v[at, rows, :] = (0.5 * both).astype(jnp.bfloat16)
            return 0

        lax.fori_loop(0, ff // ROWS, average_rows, 0)
        mixed_out(k).start()
        return 0

    lax.fori_loop(0, N_TP, average, 0)

    def drain(k, _):
        def drain_chunk(i, _):
            code_copy(i, k).wait_send()
            scale_copy(i, k).wait_send()
            stat_copy(i, k).wait_send()
            return 0

        lax.fori_loop(0, N_CHUNKS, drain_chunk, 0)
        grad_arrival(k).wait_send()
        return 0

    lax.fori_loop(1, N_TP, drain, 0)

    def drain_mixed(k, _):
        gossip_copy(k).wait_send()
        if diagonal:

            @pl.when(relays)
            def _():
                second_leg(k).wait_send()
        mixed_out(k).wait()
        return 0

    lax.fori_loop(0, N_TP, drain_mixed, 0)
    for k in range(around):
        second_leg(jnp.int32(k)).wait_send()
    normed_out.wait()


def step_at(level, nz, gate, up, target, gain, weight, rate):
    tok, ff = gate.shape
    share = target.shape[1]
    chunk = tok // N_CHUNKS
    bf16, f32, i16 = jnp.bfloat16, jnp.float32, jnp.int16
    dma = pltpu.SemaphoreType.DMA
    hbm = pl.BlockSpec(memory_space=pl.ANY)
    return pl.pallas_call(
        functools.partial(kernel, level, nz),
        out_shape=(
            jax.ShapeDtypeStruct((tok, share), bf16),
            jax.ShapeDtypeStruct(weight.shape, bf16),
        ),
        in_specs=[hbm, hbm, hbm, pl.BlockSpec(memory_space=pltpu.VMEM), hbm, pl.BlockSpec(memory_space=pltpu.SMEM)],
        out_specs=(hbm, hbm),
        scratch_shapes=[
            pltpu.VMEM((N_CHUNKS, chunk, ff), bf16),
            pltpu.VMEM((N_CHUNKS, chunk, ff), bf16),
            pltpu.VMEM((tok, share), bf16),
            pltpu.VMEM((N_TP, ff, share), bf16),
            pltpu.VMEM((N_CHUNKS, chunk, ff), bf16),
            pltpu.VMEM((ff, tok), bf16),
            pltpu.VMEM((N_TP, chunk, share), f32),
            pltpu.VMEM((chunk, 128), f32),
            pltpu.VMEM((N_CHUNKS, chunk, share), f32),
            pltpu.VMEM((N_CHUNKS, N_TP, chunk, share), i16),
            pltpu.VMEM((N_CHUNKS, 8, chunk), f32),
            pltpu.VMEM((N_CHUNKS, N_TP, chunk, share), i16),
            pltpu.VMEM((N_CHUNKS, N_TP, 8, chunk), f32),
            pltpu.VMEM((chunk, 128), f32),
            pltpu.VMEM((N_CHUNKS, 8, chunk), f32),
            pltpu.VMEM((N_CHUNKS, N_TP, 8, chunk), f32),
            pltpu.VMEM((tok, share), bf16),
            pltpu.VMEM((N_TP, tok, share), bf16),
            pltpu.VMEM((N_TP, ff, share), bf16),
            pltpu.VMEM((N_TP, ff, share), bf16),
            pltpu.VMEM((N_TP if level == 1 else RELAYED, ff, share), bf16),
            dma((3, N_CHUNKS)),
            dma((N_TP,)),
            dma((1,)),
            dma((N_TP,)),
            dma((N_CHUNKS, N_TP)),
            dma((N_CHUNKS, N_TP)),
            dma((N_CHUNKS, N_TP)),
            dma((N_CHUNKS, N_TP)),
            dma((N_CHUNKS, N_TP)),
            dma((N_CHUNKS, N_TP)),
            dma((N_TP,)),
            dma((N_TP,)),
            dma((N_TP,)),
            dma((N_TP,)),
            dma((N_TP,)),
            dma((N_TP,)),
        ],
        compiler_params=pltpu.CompilerParams(
            collective_id=level + 1, has_side_effects=True, vmem_limit_bytes=56 << 20
        ),
        name=f"step_level{level}",
    )(gate, up, target, gain, weight, rate)


def shards(nz, gate_pre, up_pre, target, norm_gain, weight, round_index):
    levels = (nz * 4).bit_length() - 1
    rate = step_rate(round_index).reshape(1)
    level = round_index[0] % levels
    operands = (gate_pre, up_pre, target, norm_gain.reshape(1, -1), weight[0], rate)
    branches = [functools.partial(step_at, number, nz) for number in range(levels)]
    normed, mixed = lax.switch(level, branches, *operands)
    return (normed, mixed[None])


def solution(mesh):
    nz = mesh.shape["dp"] // 4
    axes = ("z", "xl", "c", "y", "xh")
    finer = Mesh(mesh.devices.reshape(nz, 2, 2, N_Y, 2), axes)
    dp, tp = axes[:3], axes[3:]
    return jax.shard_map(
        functools.partial(shards, nz),
        mesh=finer,
        in_specs=(P(dp, tp), P(dp, tp), P(dp, tp), P(tp), P(dp, tp, None), P()),
        out_specs=(P(dp, tp), P(dp, tp, None)),
        check_vma=False,
    )
```

```python
import functools
import math

import jax
import jax.numpy as jnp
from jax import lax
from jax.experimental import pallas as pl
from jax.experimental.pallas import tpu as pltpu
from jax.sharding import Mesh
from jax.sharding import PartitionSpec as P

FF = 7168
EPSILON = 1e-06
CODE_MAX = 32767.0
N_CHUNKS = 3
N_TP = 8
N_Y = 4
MESH = pl.DeviceIdType.MESH
RELAYED = 2
LAG = 2
ROWS = 64


def step_rate(round_index):
    phase = (round_index[0] % 1000).astype(jnp.float32) * jnp.float32(2.0 * math.pi / 1000.0)
    return jnp.float32(0.25) * (jnp.float32(0.55) + jnp.float32(0.45) * jnp.cos(phase))


def across(rows, lanes=128):
    n = rows.shape[1]
    return jnp.broadcast_to(rows[None], (lanes // 8, 8, n)).reshape(lanes, n).T


def kernel(
    level, nz,
    gate, up, target, gain, weight, rate,
    normed, mixed,
    gate_v, up_v, target_v, w_v, h_v, ht_v, p_v, mx_v, left_v, right_v, own_v,
    ql_v, qr_v, q2_v, qs_v, rl_v, rr_v, r2_v, rs_v, tr_v, st_v, rst_v,
    norm_v, grad_v, upd_v, peer_v, relay_v,
    in_sem, w_sem, out_sem, mix_sem, qss, qrs, q2s, q2r, sss, srs, tss, trs, bss, brs, css, crs, fss, frs,
):
    share = target_v.shape[1]
    ff = w_v.shape[1]
    chunk = h_v.shape[1]
    z, xl, c, y, xh = (lax.axis_index(a) for a in ("z", "xl", "c", "y", "xh"))
    mine = y * 2 + xh

    def offset(k):
        j = lax.div(k, 2)
        return lax.rem(lax.div(j * (j + 1), 2), 4), lax.rem(k, 2)

    def member(k):
        dy, dx = offset(k)
        return lax.rem(y + dy, N_Y), lax.rem(xh + dx, 2)

    def device(k):
        py, px = member(k)
        return {"y": py, "xh": px}

    def owner(k):
        py, px = member(k)
        return py * 2 + px

    def seen_as(k):
        j = lax.div(k, 2)
        return (2 * j - 3 * lax.div(j, 2)) * 2 + lax.rem(k, 2)

    def gossip(by):
        to = lax.rem(z * 4 + xl * 2 + c + by, nz * 4)
        return {"z": lax.div(to, 4), "xl": lax.rem(lax.div(to, 2), 2), "c": lax.rem(to, 2)}

    target_device = gossip(1 << level)
    source_device = gossip(nz * 4 - (1 << level))
    diagonal = level == 1
    around = RELAYED if level == 3 and nz == 8 else 0
    if diagonal:
        sends_far = xl == 1
        relays = xl == 0
        onward = {"z": lax.rem(z + 1, nz)}
        behind = {"z": lax.rem(z + nz - 1, nz)}
        side = {"xl": 1 - xl}
    elif around:
        onward = {"z": lax.rem(z + nz - 3, nz)}
        behind = {"z": lax.rem(z + 3, nz)}

    def load(i, which):
        src, dst = ((gate, gate_v), (up, up_v))[which]
        return pltpu.make_async_copy(src.at[pl.ds(i * chunk, chunk)], dst.at[i], in_sem.at[which, i])

    def load_w(k):
        return pltpu.make_async_copy(weight.at[:, pl.ds(k * share, share)], w_v.at[k], w_sem.at[k])

    target_load = pltpu.make_async_copy(target, target_v, in_sem.at[2, 0])
    for which in range(2):
        load(0, which).start()
    for k in range(N_TP):
        load_w(k).start()
    for i in range(1, N_CHUNKS):
        for which in range(2):
            load(i, which).start()
    target_load.start()

    barrier = pltpu.get_barrier_semaphore()
    for k in range(1, N_TP):
        pl.semaphore_signal(barrier, inc=1, device_id=device(jnp.int32(k)), device_id_type=MESH)
    if diagonal:

        pl.semaphore_signal(barrier, inc=1, device_id=side, device_id_type=MESH)

        @pl.when(relays)
        def _():
            pl.semaphore_signal(barrier, inc=1, device_id=behind, device_id_type=MESH)

    else:
        pl.semaphore_signal(barrier, inc=1, device_id=source_device, device_id_type=MESH)
        if around:
            pl.semaphore_signal(barrier, inc=1, device_id=behind, device_id_type=MESH)

    half = share // 2

    def peer(d):
        return {"y": lax.rem(y + d, N_Y)} if d else {"xh": 1 - xh}

    def first_copy(i, d):
        s = (N_Y - d) % N_Y
        return pltpu.make_async_remote_copy(
            src_ref=ql_v.at[i, d - 1] if d else qr_v.at[i], dst_ref=rl_v.at[i, s - 1] if d else rr_v.at[i],
            send_sem=qss.at[i, d], recv_sem=qrs.at[i, s], device_id=peer(d), device_id_type=MESH,
        )

    def second_copy(i, d):
        s = (N_Y - d) % N_Y
        return pltpu.make_async_remote_copy(
            src_ref=q2_v.at[i, d], dst_ref=r2_v.at[i, s], send_sem=q2s.at[i, d], recv_sem=q2r.at[i, s],
            device_id=peer(d), device_id_type=MESH,
        )

    def scale_copy(stage, i, d):
        s = (N_Y - d) % N_Y
        return pltpu.make_async_remote_copy(
            src_ref=qs_v.at[stage, i], dst_ref=rs_v.at[stage, i, s],
            send_sem=sss.at[stage, i, d], recv_sem=srs.at[stage, i, s],
            device_id=peer(d), device_id_type=MESH,
        )

    def coded(values):
        return jnp.round(values).astype(jnp.int32).astype(jnp.int16)

    def decoded(codes):
        return codes.astype(jnp.int32).astype(jnp.float32)

    def send_stage(stage, i):
        for d in range(N_Y):
            scale_copy(stage, i, d).start()
            (first_copy, second_copy)[stage](i, d).start()

    def receive_stage(stage, i):
        for d in range(N_Y):
            scale_copy(stage, i, d).wait_recv()
            (first_copy, second_copy)[stage](i, d).wait_recv()
        scales = jnp.zeros((8, chunk), jnp.float32)
        for d in range(N_Y):
            scales = jnp.where(sub == d, rs_v[stage, i, d], scales)
        tr_v[...] = across(scales)

    sub = lax.broadcasted_iota(jnp.int32, (8, chunk), 0)
    lane = lax.broadcasted_iota(jnp.int32, (ROWS, 128), 1)

    def project(i, _):
        load(i, 0).wait()
        load(i, 1).wait()

        def hidden_rows(r, _):
            rows = pl.ds(r * ROWS, ROWS)
            v = gate_v[i, rows, :].astype(jnp.float32)
            h = v / (1.0 + jnp.exp(-v)) * up_v[i, rows, :].astype(jnp.float32)
            h_v[i, rows, :] = h.astype(jnp.bfloat16)
            return 0

        lax.fori_loop(0, chunk // ROWS, hidden_rows, 0)

        @pl.when(i == 0)
        def _():
            for k in range(N_TP):
                load_w(k).wait()

        mx_v[...] = jnp.zeros_like(mx_v)

        def product(k, _):
            part = jnp.dot(h_v[i], w_v[k], preferred_element_type=jnp.float32)
            p_v[k] = part
            size = jnp.abs(part)
            for half in range(share // 128):
                mx_v[...] = jnp.maximum(mx_v[...], size[:, half * 128 : (half + 1) * 128])
            return 0

        lax.fori_loop(0, N_TP, product, 0)
        largest = jnp.maximum(jnp.max(mx_v[...], axis=1, keepdims=True), 1e-30)
        mx_v[...] = jnp.broadcast_to(CODE_MAX / largest, mx_v.shape)
        qs_v[0, i] = jnp.broadcast_to(largest * (1.0 / CODE_MAX), mx_v.shape).T[0:8, :]

        @pl.when(i == 0)
        def _():
            pl.semaphore_wait(barrier, N_TP + (1 - xl if diagonal else 1 if around else 0))

        def code_rows(r, _):
            rows = pl.ds(r * ROWS, ROWS)
            inverse = mx_v[rows, :]
            for h in range(2):
                left_v[i, h, rows, :] = p_v[y * 2 + h, rows, :half]
                for d in range(1, N_Y):
                    ql_v[i, d - 1, h, rows, :] = coded(p_v[lax.rem(y + d, N_Y) * 2 + h, rows, :half] * inverse)
            for n in range(N_Y):
                right_v[i, n, rows, :] = p_v[n * 2 + xh, rows, half:]
                qr_v[i, n, rows, :] = coded(p_v[n * 2 + 1 - xh, rows, half:] * inverse)
            return 0

        lax.fori_loop(0, chunk // ROWS, code_rows, 0)
        send_stage(0, i)
        return 0

    lax.fori_loop(0, N_CHUNKS, project, 0)

    for i in range(N_CHUNKS):
        ht_v[:, i * chunk : (i + 1) * chunk] = h_v[i].T

    def combine(i, _):
        receive_stage(0, i)

        def combine_rows(r, _):
            rows = pl.ds(r * ROWS, ROWS)
            scale = tr_v[rows, :]
            for h in range(2):
                total = left_v[i, h, rows, :]
                for s in range(1, N_Y):
                    total = total + decoded(rl_v[i, s - 1, h, rows, :]) * scale[:, s : s + 1]
                left_v[i, h, rows, :] = total
            for n in range(N_Y):
                right_v[i, n, rows, :] = right_v[i, n, rows, :] + decoded(rr_v[i, n, rows, :]) * scale[:, 0:1]
            parts = [left_v[i, 1 - xh, rows, :]]
            parts += [right_v[i, lax.rem(y + d, N_Y), rows, :] for d in range(1, N_Y)]
            size = functools.reduce(jnp.maximum, [jnp.abs(part) for part in parts])
            largest = jnp.maximum(jnp.max(size, axis=1, keepdims=True), 1e-30)
            inverse = CODE_MAX / largest
            for d in range(N_Y):
                q2_v[i, d, rows, :] = coded(parts[d] * inverse)
            mx_v[rows, :] = jnp.broadcast_to(largest * (1.0 / CODE_MAX), (ROWS, 128))
            return 0

        lax.fori_loop(0, chunk // ROWS, combine_rows, 0)
        qs_v[1, i] = mx_v[...].T[0:8, :]
        send_stage(1, i)
        return 0

    lax.fori_loop(0, N_CHUNKS, combine, 0)

    def stat_copy(i, k):
        s = seen_as(k)
        return pltpu.make_async_remote_copy(
            src_ref=st_v.at[i], dst_ref=rst_v.at[i, s], send_sem=tss.at[i, k], recv_sem=trs.at[i, s],
            device_id=device(k), device_id_type=MESH,
        )

    target_load.wait()

    def reduce(i, _):
        receive_stage(1, i)

        def reduce_rows(r, _):
            rows = pl.ds(r * ROWS, ROWS)
            scale = tr_v[rows, :]
            left = left_v[i, xh, rows, :] + decoded(r2_v[i, 0, rows, :]) * scale[:, 0:1]
            right = right_v[i, y, rows, :]
            for d in range(1, N_Y):
                right = right + decoded(r2_v[i, d, rows, :]) * scale[:, d : d + 1]
            total = jnp.concatenate([left, right], axis=1)
            s = total * FF ** (-0.5)
            own_v[i, rows, :] = s
            g = gain[...]
            t = target_v[pl.ds(i * chunk + r * ROWS, ROWS), :].astype(jnp.float32)
            gs = g * s
            a = jnp.sum(s * s, axis=1, keepdims=True)
            b = jnp.sum(gs * gs, axis=1, keepdims=True)
            d = jnp.sum(gs * t, axis=1, keepdims=True)
            tr_v[rows, :] = jnp.where(lane == 0, a, jnp.where(lane == 1, b, d))
            return 0

        lax.fori_loop(0, chunk // ROWS, reduce_rows, 0)
        st_v[i] = tr_v[...].T[0:8, :]

        def send(k, _):
            stat_copy(i, k).start()
            return 0

        lax.fori_loop(1, N_TP, send, 0)
        return 0

    lax.fori_loop(0, N_CHUNKS, reduce, 0)

    width = share * N_TP

    def finish(i, _):
        sums = st_v[i]
        for k in range(1, N_TP):
            stat_copy(i, jnp.int32(k)).wait_recv()
        for k in range(1, N_TP):
            sums = sums + rst_v[i, k]
        tr_v[...] = across(sums)

        def finish_rows(r, _):
            rows = pl.ds(r * ROWS, ROWS)
            at = pl.ds(i * chunk + r * ROWS, ROWS)
            sums = tr_v[rows, :] * (1.0 / width)
            inv = lax.rsqrt(sums[:, 0:1] + EPSILON)
            inner = inv * inv * sums[:, 1:2] - inv * sums[:, 2:3]
            g = gain[...]
            normal = own_v[i, rows, :] * inv
            output = normal * g
            grad_norm = (output - target_v[at, :].astype(jnp.float32)) * g
            norm_v[at, :] = output.astype(jnp.bfloat16)
            grad_v[mine, at, :] = (inv * (grad_norm - normal * inner)).astype(jnp.bfloat16)
            return 0

        lax.fori_loop(0, chunk // ROWS, finish_rows, 0)
        return 0

    lax.fori_loop(0, N_CHUNKS, finish, 0)

    def grad_copy(which, k):
        s = seen_as(k) if which == 0 else seen_as(k) + 1
        at = owner(jnp.int32(which))
        return pltpu.make_async_remote_copy(
            src_ref=grad_v.at[at], dst_ref=grad_v.at[at], send_sem=bss.at[k + which], recv_sem=brs.at[s],
            device_id=device(k), device_id_type=MESH,
        )

    def grad_arrival(k):
        at = owner(k)
        return pltpu.make_async_remote_copy(
            src_ref=grad_v.at[at], dst_ref=grad_v.at[at], send_sem=bss.at[k], recv_sem=brs.at[k],
            device_id=device(k), device_id_type=MESH,
        )

    for k in (1, 2, 4, 6):
        grad_copy(0, jnp.int32(k)).start()
    normed_out = pltpu.make_async_copy(norm_v, normed, out_sem.at[0])
    normed_out.start()

    def gossip_copy(k):
        at = owner(k)
        return pltpu.make_async_remote_copy(
            src_ref=upd_v.at[at], dst_ref=peer_v.at[at], send_sem=css.at[k], recv_sem=crs.at[k],
            device_id=target_device, device_id_type=MESH,
        )

    def first_leg(k):
        at = owner(k)
        return pltpu.make_async_remote_copy(
            src_ref=upd_v.at[at], dst_ref=relay_v.at[k], send_sem=css.at[k], recv_sem=frs.at[k],
            device_id=side if diagonal else onward, device_id_type=MESH,
        )

    def second_leg(k):
        at = owner(k)
        return pltpu.make_async_remote_copy(
            src_ref=relay_v.at[k], dst_ref=peer_v.at[at], send_sem=fss.at[k], recv_sem=crs.at[k],
            device_id=onward, device_id_type=MESH,
        )

    def forward(k):
        first_leg(k).wait_recv()
        second_leg(k).start()

    def send_updated(k):
        if diagonal:

            @pl.when(sends_far)
            def _():
                first_leg(k).start()

            @pl.when(jnp.logical_not(sends_far))
            def _():
                gossip_copy(k).start()

            @pl.when(jnp.logical_and(relays, k >= LAG))
            def _():
                forward(k - LAG)

        elif around:

            @pl.when(k < around)
            def _():
                first_leg(k).start()

            @pl.when(k >= around)
            def _():
                gossip_copy(k).start()

        else:
            gossip_copy(k).start()

    step = rate[0]

    def update(k, _):
        at = owner(k)

        @pl.when(k > 0)
        def _():
            grad_arrival(k).wait_recv()

        @pl.when(k == 1)
        def _():
            for j in (2, 4, 6):
                grad_copy(1, jnp.int32(j)).start()

        weight_grad = jnp.dot(ht_v[...], grad_v[at], preferred_element_type=jnp.float32) * FF ** (-0.5)
        upd_v[at] = (w_v[at].astype(jnp.float32) - step * weight_grad).astype(jnp.bfloat16)
        send_updated(k)
        return 0

    lax.fori_loop(0, N_TP, update, 0)
    if diagonal:

        @pl.when(relays)
        def _():
            for k in range(N_TP - LAG, N_TP):
                forward(jnp.int32(k))

    for k in range(around):
        forward(jnp.int32(k))

    def mixed_out(k):
        at = owner(k)
        return pltpu.make_async_copy(
            w_v.at[at], mixed.at[:, pl.ds(pl.multiple_of(at * share, share), share)], mix_sem.at[k]
        )

    def average(number, _):
        k = lax.rem(number + around, N_TP)
        at = owner(k)
        gossip_copy(k).wait_recv()

        def average_rows(r, _):
            rows = pl.ds(r * ROWS, ROWS)
            both = upd_v[at, rows, :].astype(jnp.float32) + peer_v[at, rows, :].astype(jnp.float32)
            w_v[at, rows, :] = (0.5 * both).astype(jnp.bfloat16)
            return 0

        lax.fori_loop(0, ff // ROWS, average_rows, 0)
        mixed_out(k).start()
        return 0

    lax.fori_loop(0, N_TP, average, 0)

    def drain(k, _):
        def drain_chunk(i, _):
            stat_copy(i, k).wait_send()
            return 0

        lax.fori_loop(0, N_CHUNKS, drain_chunk, 0)
        grad_arrival(k).wait_send()
        return 0

    lax.fori_loop(1, N_TP, drain, 0)

    def drain_stages(i, _):
        for d in range(N_Y):
            first_copy(i, d).wait_send()
            second_copy(i, d).wait_send()
            for stage in range(2):
                scale_copy(stage, i, d).wait_send()
        return 0

    lax.fori_loop(0, N_CHUNKS, drain_stages, 0)

    def drain_mixed(k, _):
        gossip_copy(k).wait_send()
        if diagonal:

            @pl.when(relays)
            def _():
                second_leg(k).wait_send()
        mixed_out(k).wait()
        return 0

    lax.fori_loop(0, N_TP, drain_mixed, 0)
    for k in range(around):
        second_leg(jnp.int32(k)).wait_send()
    normed_out.wait()


def step_at(level, nz, gate, up, target, gain, weight, rate):
    tok, ff = gate.shape
    share = target.shape[1]
    chunk = tok // N_CHUNKS
    bf16, f32, i16 = jnp.bfloat16, jnp.float32, jnp.int16
    dma = pltpu.SemaphoreType.DMA
    hbm = pl.BlockSpec(memory_space=pl.ANY)
    return pl.pallas_call(
        functools.partial(kernel, level, nz),
        out_shape=(
            jax.ShapeDtypeStruct((tok, share), bf16),
            jax.ShapeDtypeStruct(weight.shape, bf16),
        ),
        in_specs=[hbm, hbm, hbm, pl.BlockSpec(memory_space=pltpu.VMEM), hbm, pl.BlockSpec(memory_space=pltpu.SMEM)],
        out_specs=(hbm, hbm),
        scratch_shapes=[
            pltpu.VMEM((N_CHUNKS, chunk, ff), bf16),
            pltpu.VMEM((N_CHUNKS, chunk, ff), bf16),
            pltpu.VMEM((tok, share), bf16),
            pltpu.VMEM((N_TP, ff, share), bf16),
            pltpu.VMEM((N_CHUNKS, chunk, ff), bf16),
            pltpu.VMEM((ff, tok), bf16),
            pltpu.VMEM((N_TP, chunk, share), f32),
            pltpu.VMEM((chunk, 128), f32),
            pltpu.VMEM((N_CHUNKS, 2, chunk, share // 2), f32),
            pltpu.VMEM((N_CHUNKS, N_Y, chunk, share // 2), f32),
            pltpu.VMEM((N_CHUNKS, chunk, share), f32),
            pltpu.VMEM((N_CHUNKS, N_Y - 1, 2, chunk, share // 2), i16),
            pltpu.VMEM((N_CHUNKS, N_Y, chunk, share // 2), i16),
            pltpu.VMEM((N_CHUNKS, N_Y, chunk, share // 2), i16),
            pltpu.VMEM((2, N_CHUNKS, 8, chunk), f32),
            pltpu.VMEM((N_CHUNKS, N_Y - 1, 2, chunk, share // 2), i16),
            pltpu.VMEM((N_CHUNKS, N_Y, chunk, share // 2), i16),
            pltpu.VMEM((N_CHUNKS, N_Y, chunk, share // 2), i16),
            pltpu.VMEM((2, N_CHUNKS, N_Y, 8, chunk), f32),
            pltpu.VMEM((chunk, 128), f32),
            pltpu.VMEM((N_CHUNKS, 8, chunk), f32),
            pltpu.VMEM((N_CHUNKS, N_TP, 8, chunk), f32),
            pltpu.VMEM((tok, share), bf16),
            pltpu.VMEM((N_TP, tok, share), bf16),
            pltpu.VMEM((N_TP, ff, share), bf16),
            pltpu.VMEM((N_TP, ff, share), bf16),
            pltpu.VMEM((N_TP if level == 1 else RELAYED, ff, share), bf16),
            dma((3, N_CHUNKS)),
            dma((N_TP,)),
            dma((1,)),
            dma((N_TP,)),
            dma((N_CHUNKS, N_Y)),
            dma((N_CHUNKS, N_Y)),
            dma((N_CHUNKS, N_Y)),
            dma((N_CHUNKS, N_Y)),
            dma((2, N_CHUNKS, N_Y)),
            dma((2, N_CHUNKS, N_Y)),
            dma((N_CHUNKS, N_TP)),
            dma((N_CHUNKS, N_TP)),
            dma((N_TP,)),
            dma((N_TP,)),
            dma((N_TP,)),
            dma((N_TP,)),
            dma((N_TP,)),
            dma((N_TP,)),
        ],
        compiler_params=pltpu.CompilerParams(
            collective_id=level + 1, has_side_effects=True, vmem_limit_bytes=56 << 20
        ),
        name=f"step_level{level}",
    )(gate, up, target, gain, weight, rate)


def shards(nz, gate_pre, up_pre, target, norm_gain, weight, round_index):
    levels = (nz * 4).bit_length() - 1
    rate = step_rate(round_index).reshape(1)
    level = round_index[0] % levels
    operands = (gate_pre, up_pre, target, norm_gain.reshape(1, -1), weight[0], rate)
    branches = [functools.partial(step_at, number, nz) for number in range(levels)]
    normed, mixed = lax.switch(level, branches, *operands)
    return (normed, mixed[None])


def solution(mesh):
    nz = mesh.shape["dp"] // 4
    axes = ("z", "xl", "c", "y", "xh")
    finer = Mesh(mesh.devices.reshape(nz, 2, 2, N_Y, 2), axes)
    dp, tp = axes[:3], axes[3:]
    return jax.shard_map(
        functools.partial(shards, nz),
        mesh=finer,
        in_specs=(P(dp, tp), P(dp, tp), P(dp, tp), P(tp), P(dp, tp, None), P()),
        out_specs=(P(dp, tp), P(dp, tp, None)),
        check_vma=False,
    )
```

```python
import functools
import math

import jax
import jax.numpy as jnp
from jax import lax
from jax.experimental import pallas as pl
from jax.experimental.pallas import tpu as pltpu
from jax.sharding import Mesh
from jax.sharding import PartitionSpec as P

FF = 7168
EPSILON = 1e-06
CODE_MAX = 32767.0
N_CHUNKS = 3
N_TP = 8
N_Y = 4
MESH = pl.DeviceIdType.MESH
RELAYED = 2
EARLY = {2: 384, 3: 176, 4: 176}
LAG = 2
ROWS = 64


def step_rate(round_index):
    phase = (round_index[0] % 1000).astype(jnp.float32) * jnp.float32(2.0 * math.pi / 1000.0)
    return jnp.float32(0.25) * (jnp.float32(0.55) + jnp.float32(0.45) * jnp.cos(phase))


def across(rows, lanes=128):
    n = rows.shape[1]
    return jnp.broadcast_to(rows[None], (lanes // 8, 8, n)).reshape(lanes, n).T


def kernel(
    level, nz, early,
    gate, up, target, gain, weight, rate,
    normed, mixed,
    gate_v, up_v, target_v, w_v, h_v, ht_v, p_v, mx_v, left_v, right_v, own_v,
    ql_v, qr_v, q2_v, qs_v, rl_v, rr_v, r2_v, rs_v, tr_v, st_v, rst_v,
    norm_v, grad_v, their_grad_v, their_ht_v, upd_v, peer_v, relay_v,
    in_sem, w_sem, out_sem, mix_sem, qss, qrs, q2s, q2r, sss, srs, tss, trs, bss, brs, css, crs, fss, frs, ess, ers,
):
    share = target_v.shape[1]
    ff = w_v.shape[1]
    chunk = h_v.shape[1]
    z, xl, c, y, xh = (lax.axis_index(a) for a in ("z", "xl", "c", "y", "xh"))
    mine = y * 2 + xh

    def offset(k):
        j = lax.div(k, 2)
        return lax.rem(lax.div(j * (j + 1), 2), 4), lax.rem(k, 2)

    def member(k):
        dy, dx = offset(k)
        return lax.rem(y + dy, N_Y), lax.rem(xh + dx, 2)

    def device(k):
        py, px = member(k)
        return {"y": py, "xh": px}

    def owner(k):
        py, px = member(k)
        return py * 2 + px

    def seen_as(k):
        j = lax.div(k, 2)
        return (2 * j - 3 * lax.div(j, 2)) * 2 + lax.rem(k, 2)

    def gossip(by):
        to = lax.rem(z * 4 + xl * 2 + c + by, nz * 4)
        return {"z": lax.div(to, 4), "xl": lax.rem(lax.div(to, 2), 2), "c": lax.rem(to, 2)}

    target_device = gossip(1 << level)
    source_device = gossip(nz * 4 - (1 << level))
    diagonal = level < 2
    around = RELAYED if level == 3 and nz == 8 else 0
    if diagonal:
        sends_far = jnp.logical_and(xl == 1, c == 1) if level == 0 else xl == 1
        relays = jnp.logical_and(xl == 0, c == 0) if level == 0 else xl == 0
        relay_count = (1 - xl) * (1 - c) if level == 0 else 1 - xl
        onward = {"z": lax.rem(z + 1, nz)}
        behind = {"z": lax.rem(z + nz - 1, nz)}
        side = {"xl": 1 - xl, "c": 1 - c} if level == 0 else {"xl": 1 - xl}
    elif around:
        onward = {"z": lax.rem(z + nz - 3, nz)}
        behind = {"z": lax.rem(z + 3, nz)}

    def load(i, which):
        src, dst = ((gate, gate_v), (up, up_v))[which]
        return pltpu.make_async_copy(src.at[pl.ds(i * chunk, chunk)], dst.at[i], in_sem.at[which, i])

    def load_w(k):
        return pltpu.make_async_copy(weight.at[:, pl.ds(k * share, share)], w_v.at[k], w_sem.at[k])

    target_load = pltpu.make_async_copy(target, target_v, in_sem.at[2, 0])
    for which in range(2):
        load(0, which).start()
    for k in range(N_TP):
        load_w(k).start()
    for i in range(1, N_CHUNKS):
        for which in range(2):
            load(i, which).start()
    target_load.start()

    barrier = pltpu.get_barrier_semaphore()
    for k in range(1, N_TP):
        pl.semaphore_signal(barrier, inc=1, device_id=device(jnp.int32(k)), device_id_type=MESH)
    if diagonal:

        @pl.when(relays)
        def _():
            pl.semaphore_signal(barrier, inc=1, device_id=side, device_id_type=MESH)
            pl.semaphore_signal(barrier, inc=1, device_id=behind, device_id_type=MESH)

        @pl.when(jnp.logical_not(relays))
        def _():
            pl.semaphore_signal(barrier, inc=1, device_id=source_device, device_id_type=MESH)

    else:
        pl.semaphore_signal(barrier, inc=1, device_id=source_device, device_id_type=MESH)
        if around:
            pl.semaphore_signal(barrier, inc=1, device_id=behind, device_id_type=MESH)

    half = share // 2

    def peer(d):
        return {"y": lax.rem(y + d, N_Y)} if d else {"xh": 1 - xh}

    def first_copy(i, d):
        s = (N_Y - d) % N_Y
        return pltpu.make_async_remote_copy(
            src_ref=ql_v.at[i, d - 1] if d else qr_v.at[i], dst_ref=rl_v.at[i, s - 1] if d else rr_v.at[i],
            send_sem=qss.at[i, d], recv_sem=qrs.at[i, s], device_id=peer(d), device_id_type=MESH,
        )

    def second_copy(i, d):
        s = (N_Y - d) % N_Y
        return pltpu.make_async_remote_copy(
            src_ref=q2_v.at[i, d], dst_ref=r2_v.at[i, s], send_sem=q2s.at[i, d], recv_sem=q2r.at[i, s],
            device_id=peer(d), device_id_type=MESH,
        )

    def scale_copy(stage, i, d):
        s = (N_Y - d) % N_Y
        return pltpu.make_async_remote_copy(
            src_ref=qs_v.at[stage, i], dst_ref=rs_v.at[stage, i, s],
            send_sem=sss.at[stage, i, d], recv_sem=srs.at[stage, i, s],
            device_id=peer(d), device_id_type=MESH,
        )

    def coded(values):
        return jnp.round(values).astype(jnp.int32).astype(jnp.int16)

    def decoded(codes):
        return codes.astype(jnp.int32).astype(jnp.float32)

    def send_stage(stage, i):
        for d in range(N_Y):
            scale_copy(stage, i, d).start()
            (first_copy, second_copy)[stage](i, d).start()

    def receive_stage(stage, i):
        for d in range(N_Y):
            scale_copy(stage, i, d).wait_recv()
            (first_copy, second_copy)[stage](i, d).wait_recv()
        scales = jnp.zeros((8, chunk), jnp.float32)
        for d in range(N_Y):
            scales = jnp.where(sub == d, rs_v[stage, i, d], scales)
        tr_v[...] = across(scales)

    sub = lax.broadcasted_iota(jnp.int32, (8, chunk), 0)
    lane = lax.broadcasted_iota(jnp.int32, (ROWS, 128), 1)

    def early_copy(n):
        rows = pl.ds(0, early)
        src, dst = (
            (w_v.at[:, rows], peer_v.at[:, rows]),
            (ht_v.at[rows], their_ht_v),
            (grad_v.at[mine], their_grad_v.at[mine]),
        )[n]
        return pltpu.make_async_remote_copy(
            src_ref=src, dst_ref=dst, send_sem=ess.at[n], recv_sem=ers.at[n],
            device_id=target_device, device_id_type=MESH,
        )

    def project(i, _):
        load(i, 0).wait()
        load(i, 1).wait()

        def hidden_rows(r, _):
            rows = pl.ds(r * ROWS, ROWS)
            v = gate_v[i, rows, :].astype(jnp.float32)
            h = v / (1.0 + jnp.exp(-v)) * up_v[i, rows, :].astype(jnp.float32)
            h_v[i, rows, :] = h.astype(jnp.bfloat16)
            return 0

        lax.fori_loop(0, chunk // ROWS, hidden_rows, 0)

        @pl.when(i == 0)
        def _():
            for k in range(N_TP):
                load_w(k).wait()
            pl.semaphore_wait(barrier, N_TP + (relay_count if diagonal else 1 if around else 0))
            if early:
                early_copy(0).start()

        mx_v[...] = jnp.zeros_like(mx_v)

        def product(k, _):
            part = jnp.dot(h_v[i], w_v[k], preferred_element_type=jnp.float32)
            p_v[k] = part
            size = jnp.abs(part)
            for half in range(share // 128):
                mx_v[...] = jnp.maximum(mx_v[...], size[:, half * 128 : (half + 1) * 128])
            return 0

        lax.fori_loop(0, N_TP, product, 0)
        largest = jnp.maximum(jnp.max(mx_v[...], axis=1, keepdims=True), 1e-30)
        mx_v[...] = jnp.broadcast_to(CODE_MAX / largest, mx_v.shape)
        qs_v[0, i] = jnp.broadcast_to(largest * (1.0 / CODE_MAX), mx_v.shape).T[0:8, :]

        def code_rows(r, _):
            rows = pl.ds(r * ROWS, ROWS)
            inverse = mx_v[rows, :]
            for h in range(2):
                left_v[i, h, rows, :] = p_v[y * 2 + h, rows, :half]
                for d in range(1, N_Y):
                    ql_v[i, d - 1, h, rows, :] = coded(p_v[lax.rem(y + d, N_Y) * 2 + h, rows, :half] * inverse)
            for n in range(N_Y):
                right_v[i, n, rows, :] = p_v[n * 2 + xh, rows, half:]
                qr_v[i, n, rows, :] = coded(p_v[n * 2 + 1 - xh, rows, half:] * inverse)
            return 0

        lax.fori_loop(0, chunk // ROWS, code_rows, 0)
        send_stage(0, i)
        return 0

    lax.fori_loop(0, N_CHUNKS, project, 0)

    for i in range(N_CHUNKS):
        ht_v[:, i * chunk : (i + 1) * chunk] = h_v[i].T
    if early:
        early_copy(1).start()

    def combine(i, _):
        receive_stage(0, i)

        def combine_rows(r, _):
            rows = pl.ds(r * ROWS, ROWS)
            scale = tr_v[rows, :]
            for h in range(2):
                total = left_v[i, h, rows, :]
                for s in range(1, N_Y):
                    total = total + decoded(rl_v[i, s - 1, h, rows, :]) * scale[:, s : s + 1]
                left_v[i, h, rows, :] = total
            for n in range(N_Y):
                right_v[i, n, rows, :] = right_v[i, n, rows, :] + decoded(rr_v[i, n, rows, :]) * scale[:, 0:1]
            parts = [left_v[i, 1 - xh, rows, :]]
            parts += [right_v[i, lax.rem(y + d, N_Y), rows, :] for d in range(1, N_Y)]
            size = functools.reduce(jnp.maximum, [jnp.abs(part) for part in parts])
            largest = jnp.maximum(jnp.max(size, axis=1, keepdims=True), 1e-30)
            inverse = CODE_MAX / largest
            for d in range(N_Y):
                q2_v[i, d, rows, :] = coded(parts[d] * inverse)
            mx_v[rows, :] = jnp.broadcast_to(largest * (1.0 / CODE_MAX), (ROWS, 128))
            return 0

        lax.fori_loop(0, chunk // ROWS, combine_rows, 0)
        qs_v[1, i] = mx_v[...].T[0:8, :]
        send_stage(1, i)
        return 0

    lax.fori_loop(0, N_CHUNKS, combine, 0)

    def stat_copy(i, k):
        s = seen_as(k)
        return pltpu.make_async_remote_copy(
            src_ref=st_v.at[i], dst_ref=rst_v.at[i, s], send_sem=tss.at[i, k], recv_sem=trs.at[i, s],
            device_id=device(k), device_id_type=MESH,
        )

    target_load.wait()

    def reduce(i, _):
        receive_stage(1, i)

        def reduce_rows(r, _):
            rows = pl.ds(r * ROWS, ROWS)
            scale = tr_v[rows, :]
            left = left_v[i, xh, rows, :] + decoded(r2_v[i, 0, rows, :]) * scale[:, 0:1]
            right = right_v[i, y, rows, :]
            for d in range(1, N_Y):
                right = right + decoded(r2_v[i, d, rows, :]) * scale[:, d : d + 1]
            total = jnp.concatenate([left, right], axis=1)
            s = total * FF ** (-0.5)
            own_v[i, rows, :] = s
            g = gain[...]
            t = target_v[pl.ds(i * chunk + r * ROWS, ROWS), :].astype(jnp.float32)
            gs = g * s
            a = jnp.sum(s * s, axis=1, keepdims=True)
            b = jnp.sum(gs * gs, axis=1, keepdims=True)
            d = jnp.sum(gs * t, axis=1, keepdims=True)
            tr_v[rows, :] = jnp.where(lane == 0, a, jnp.where(lane == 1, b, d))
            return 0

        lax.fori_loop(0, chunk // ROWS, reduce_rows, 0)
        st_v[i] = tr_v[...].T[0:8, :]

        def send(k, _):
            stat_copy(i, k).start()
            return 0

        lax.fori_loop(1, N_TP, send, 0)
        return 0

    lax.fori_loop(0, N_CHUNKS, reduce, 0)

    width = share * N_TP

    def finish(i, _):
        sums = st_v[i]
        for k in range(1, N_TP):
            stat_copy(i, jnp.int32(k)).wait_recv()
        for k in range(1, N_TP):
            sums = sums + rst_v[i, k]
        tr_v[...] = across(sums)

        def finish_rows(r, _):
            rows = pl.ds(r * ROWS, ROWS)
            at = pl.ds(i * chunk + r * ROWS, ROWS)
            sums = tr_v[rows, :] * (1.0 / width)
            inv = lax.rsqrt(sums[:, 0:1] + EPSILON)
            inner = inv * inv * sums[:, 1:2] - inv * sums[:, 2:3]
            g = gain[...]
            normal = own_v[i, rows, :] * inv
            output = normal * g
            grad_norm = (output - target_v[at, :].astype(jnp.float32)) * g
            norm_v[at, :] = output.astype(jnp.bfloat16)
            grad_v[mine, at, :] = (inv * (grad_norm - normal * inner)).astype(jnp.bfloat16)
            return 0

        lax.fori_loop(0, chunk // ROWS, finish_rows, 0)
        return 0

    lax.fori_loop(0, N_CHUNKS, finish, 0)

    token_half = grad_v.shape[1] // 2

    def share_copy(b, which, k):
        buf = (grad_v, their_grad_v)[b]
        at = owner(jnp.int32(which))
        return pltpu.make_async_remote_copy(
            src_ref=buf.at[at], dst_ref=buf.at[at], send_sem=bss.at[b, k + which], recv_sem=brs.at[b, seen_as(k) + which],
            device_id=device(k), device_id_type=MESH,
        )

    def passed_on(b, k):
        buf = (grad_v, their_grad_v)[b]
        j = lax.div(k, 2)
        h = 2 - j
        part = buf.at[owner(k), pl.ds(pl.multiple_of(h * token_half, token_half), token_half)]
        sem = N_TP - 2 + lax.rem(k, 2) + 2 * h
        return pltpu.make_async_remote_copy(
            src_ref=part, dst_ref=part, send_sem=bss.at[b, sem], recv_sem=brs.at[b, sem],
            device_id={"y": lax.rem(y + N_Y + 1 - 2 * j, N_Y)}, device_id_type=MESH,
        )

    def near_arrival(b, k):
        buf = (grad_v, their_grad_v)[b]
        at = owner(k)
        return pltpu.make_async_remote_copy(
            src_ref=buf.at[at], dst_ref=buf.at[at], send_sem=bss.at[b, k], recv_sem=brs.at[b, k],
            device_id=device(k), device_id_type=MESH,
        )

    def far_arrival(b, k, h):
        buf = (grad_v, their_grad_v)[b]
        part = buf.at[owner(k), pl.ds(h * token_half, token_half)]
        return pltpu.make_async_remote_copy(
            src_ref=part, dst_ref=part, send_sem=bss.at[b, k + 2 * h], recv_sem=brs.at[b, k + 2 * h],
            device_id=device(k), device_id_type=MESH,
        )

    def send_own(b):
        for k in (1, 2, 4):
            share_copy(b, 0, jnp.int32(k)).start()

    def receive_near(b, k):
        near_arrival(b, k).wait_recv()

        @pl.when(k == 1)
        def _():
            for j in (2, 4):
                share_copy(b, 1, jnp.int32(j)).start()

        @pl.when(k > 1)
        def _():
            passed_on(b, k).start()

    def receive_far(b, k):
        for h in range(2):
            far_arrival(b, k, h).wait_recv()

    send_own(0)
    if early:
        early_copy(2).start()
    normed_out = pltpu.make_async_copy(norm_v, normed, out_sem.at[0])
    normed_out.start()

    late = pl.ds(early, ff - early)

    def gossip_copy(k):
        at = owner(k)
        return pltpu.make_async_remote_copy(
            src_ref=upd_v.at[at, late], dst_ref=peer_v.at[at, late], send_sem=css.at[k], recv_sem=crs.at[k],
            device_id=target_device, device_id_type=MESH,
        )

    def first_leg(k):
        at = owner(k)
        return pltpu.make_async_remote_copy(
            src_ref=upd_v.at[at, late], dst_ref=relay_v.at[k], send_sem=css.at[k], recv_sem=frs.at[k],
            device_id=side if diagonal else onward, device_id_type=MESH,
        )

    def second_leg(k):
        at = owner(k)
        return pltpu.make_async_remote_copy(
            src_ref=relay_v.at[k], dst_ref=peer_v.at[at, late], send_sem=fss.at[k], recv_sem=crs.at[k],
            device_id=onward, device_id_type=MESH,
        )

    def forward(k):
        first_leg(k).wait_recv()
        second_leg(k).start()

    def send_updated(k):
        if diagonal:

            @pl.when(sends_far)
            def _():
                first_leg(k).start()

            @pl.when(jnp.logical_not(sends_far))
            def _():
                gossip_copy(k).start()

            @pl.when(jnp.logical_and(relays, k >= LAG))
            def _():
                forward(k - LAG)

        elif around:

            @pl.when(k < around)
            def _():
                first_leg(k).start()

            @pl.when(k >= around)
            def _():
                gossip_copy(k).start()

        else:
            gossip_copy(k).start()

    step = rate[0]

    def update(k, _):
        at = owner(k)

        @pl.when(jnp.logical_and(k > 0, k < N_TP - 2))
        def _():
            receive_near(0, k)

        @pl.when(k >= N_TP - 2)
        def _():
            receive_far(0, k)

        weight_grad = jnp.dot(ht_v[...], grad_v[at], preferred_element_type=jnp.float32) * FF ** (-0.5)
        upd_v[at] = (w_v[at].astype(jnp.float32) - step * weight_grad).astype(jnp.bfloat16)
        send_updated(k)
        return 0

    lax.fori_loop(0, N_TP, update, 0)
    if diagonal:

        @pl.when(relays)
        def _():
            for k in range(N_TP - LAG, N_TP):
                forward(jnp.int32(k))

    if early:
        early_copy(2).wait_recv()
        send_own(1)

        def pass_theirs(k, _):
            receive_near(1, k)
            return 0

        lax.fori_loop(1, N_TP - 2, pass_theirs, 0)
        early_copy(0).wait()
        early_copy(1).wait()
    for k in range(around):
        forward(jnp.int32(k))

    def mixed_out(k):
        at = owner(k)
        return pltpu.make_async_copy(
            w_v.at[at], mixed.at[:, pl.ds(pl.multiple_of(at * share, share), share)], mix_sem.at[k]
        )

    def average(number, _):
        k = lax.rem(number + around, N_TP)
        at = owner(k)
        if early:

            @pl.when(k >= N_TP - 2)
            def _():
                receive_far(1, k)

            weight_grad = jnp.dot(their_ht_v[...], their_grad_v[at], preferred_element_type=jnp.float32) * FF ** (-0.5)
            theirs = peer_v[at, :early, :].astype(jnp.float32) - step * weight_grad
            peer_v[at, :early, :] = theirs.astype(jnp.bfloat16)
        gossip_copy(k).wait_recv()

        def average_rows(r, _):
            rows = pl.ds(r * ROWS, ROWS)
            both = upd_v[at, rows, :].astype(jnp.float32) + peer_v[at, rows, :].astype(jnp.float32)
            w_v[at, rows, :] = (0.5 * both).astype(jnp.bfloat16)
            return 0

        lax.fori_loop(0, ff // ROWS, average_rows, 0)
        mixed_out(k).start()
        return 0

    lax.fori_loop(0, N_TP, average, 0)

    def drain(k, _):
        def drain_chunk(i, _):
            stat_copy(i, k).wait_send()
            return 0

        lax.fori_loop(0, N_CHUNKS, drain_chunk, 0)
        return 0

    lax.fori_loop(1, N_TP, drain, 0)

    def drain_shares(k, _):
        for b in range(2 if early else 1):
            near_arrival(b, k).wait_send()
        return 0

    lax.fori_loop(1, N_TP - 2, drain_shares, 0)
    for k in (N_TP - 2, N_TP - 1):
        for h in range(2):
            for b in range(2 if early else 1):
                far_arrival(b, jnp.int32(k), h).wait_send()
    if early:
        early_copy(2).wait_send()

    def drain_stages(i, _):
        for d in range(N_Y):
            first_copy(i, d).wait_send()
            second_copy(i, d).wait_send()
            for stage in range(2):
                scale_copy(stage, i, d).wait_send()
        return 0

    lax.fori_loop(0, N_CHUNKS, drain_stages, 0)

    def drain_mixed(k, _):
        gossip_copy(k).wait_send()
        if diagonal:

            @pl.when(relays)
            def _():
                second_leg(k).wait_send()
        mixed_out(k).wait()
        return 0

    lax.fori_loop(0, N_TP, drain_mixed, 0)
    for k in range(around):
        second_leg(jnp.int32(k)).wait_send()
    normed_out.wait()


def step_at(level, nz, gate, up, target, gain, weight, rate):
    tok, ff = gate.shape
    share = target.shape[1]
    chunk = tok // N_CHUNKS
    early = EARLY.get(level, 0) if (nz, ff) == (8, 896) else 0
    bf16, f32, i16 = jnp.bfloat16, jnp.float32, jnp.int16
    dma = pltpu.SemaphoreType.DMA
    hbm = pl.BlockSpec(memory_space=pl.ANY)
    return pl.pallas_call(
        functools.partial(kernel, level, nz, early),
        out_shape=(
            jax.ShapeDtypeStruct((tok, share), bf16),
            jax.ShapeDtypeStruct(weight.shape, bf16),
        ),
        in_specs=[hbm, hbm, hbm, pl.BlockSpec(memory_space=pltpu.VMEM), hbm, pl.BlockSpec(memory_space=pltpu.SMEM)],
        out_specs=(hbm, hbm),
        scratch_shapes=[
            pltpu.VMEM((N_CHUNKS, chunk, ff), bf16),
            pltpu.VMEM((N_CHUNKS, chunk, ff), bf16),
            pltpu.VMEM((tok, share), bf16),
            pltpu.VMEM((N_TP, ff, share), bf16),
            pltpu.VMEM((N_CHUNKS, chunk, ff), bf16),
            pltpu.VMEM((ff, tok), bf16),
            pltpu.VMEM((N_TP, chunk, share), f32),
            pltpu.VMEM((chunk, 128), f32),
            pltpu.VMEM((N_CHUNKS, 2, chunk, share // 2), f32),
            pltpu.VMEM((N_CHUNKS, N_Y, chunk, share // 2), f32),
            pltpu.VMEM((N_CHUNKS, chunk, share), f32),
            pltpu.VMEM((N_CHUNKS, N_Y - 1, 2, chunk, share // 2), i16),
            pltpu.VMEM((N_CHUNKS, N_Y, chunk, share // 2), i16),
            pltpu.VMEM((N_CHUNKS, N_Y, chunk, share // 2), i16),
            pltpu.VMEM((2, N_CHUNKS, 8, chunk), f32),
            pltpu.VMEM((N_CHUNKS, N_Y - 1, 2, chunk, share // 2), i16),
            pltpu.VMEM((N_CHUNKS, N_Y, chunk, share // 2), i16),
            pltpu.VMEM((N_CHUNKS, N_Y, chunk, share // 2), i16),
            pltpu.VMEM((2, N_CHUNKS, N_Y, 8, chunk), f32),
            pltpu.VMEM((chunk, 128), f32),
            pltpu.VMEM((N_CHUNKS, 8, chunk), f32),
            pltpu.VMEM((N_CHUNKS, N_TP, 8, chunk), f32),
            pltpu.VMEM((tok, share), bf16),
            pltpu.VMEM((N_TP, tok, share), bf16),
            pltpu.VMEM((N_TP, tok if early else 16, share), bf16),
            pltpu.VMEM((max(early, 16), tok), bf16),
            pltpu.VMEM((N_TP, ff, share), bf16),
            pltpu.VMEM((N_TP, ff, share), bf16),
            pltpu.VMEM((N_TP if level < 2 else RELAYED, ff - early, share), bf16),
            dma((3, N_CHUNKS)),
            dma((N_TP,)),
            dma((1,)),
            dma((N_TP,)),
            dma((N_CHUNKS, N_Y)),
            dma((N_CHUNKS, N_Y)),
            dma((N_CHUNKS, N_Y)),
            dma((N_CHUNKS, N_Y)),
            dma((2, N_CHUNKS, N_Y)),
            dma((2, N_CHUNKS, N_Y)),
            dma((N_CHUNKS, N_TP)),
            dma((N_CHUNKS, N_TP)),
            dma((2, N_TP + 2)),
            dma((2, N_TP + 2)),
            dma((N_TP,)),
            dma((N_TP,)),
            dma((N_TP,)),
            dma((N_TP,)),
            dma((3,)),
            dma((3,)),
        ],
        compiler_params=pltpu.CompilerParams(
            collective_id=level + 1, has_side_effects=True, vmem_limit_bytes=56 << 20
        ),
        name=f"step_level{level}",
    )(gate, up, target, gain, weight, rate)


def shards(nz, gate_pre, up_pre, target, norm_gain, weight, round_index):
    levels = (nz * 4).bit_length() - 1
    rate = step_rate(round_index).reshape(1)
    level = round_index[0] % levels
    operands = (gate_pre, up_pre, target, norm_gain.reshape(1, -1), weight[0], rate)
    branches = [functools.partial(step_at, number, nz) for number in range(levels)]
    normed, mixed = lax.switch(level, branches, *operands)
    return (normed, mixed[None])


def solution(mesh):
    nz = mesh.shape["dp"] // 4
    axes = ("z", "xl", "c", "y", "xh")
    finer = Mesh(mesh.devices.reshape(nz, 2, 2, N_Y, 2), axes)
    dp, tp = axes[:3], axes[3:]
    return jax.shard_map(
        functools.partial(shards, nz),
        mesh=finer,
        in_specs=(P(dp, tp), P(dp, tp), P(dp, tp), P(tp), P(dp, tp, None), P()),
        out_specs=(P(dp, tp), P(dp, tp, None)),
        check_vma=False,
    )
```

```python
import functools
import math

import jax
import jax.numpy as jnp
from jax import lax
from jax.experimental import pallas as pl
from jax.experimental.pallas import tpu as pltpu
from jax.sharding import Mesh
from jax.sharding import PartitionSpec as P

FF = 7168
EPSILON = 1e-06
CODE_MAX = 32767.0
N_CHUNKS = 3
N_TP = 8
N_Y = 4
MESH = pl.DeviceIdType.MESH
RELAYED = 2
EARLY = {2: 384, 3: 176, 4: 176}
PIECES = 4
LAG = 2
ROWS = 64


def step_rate(round_index):
    phase = (round_index[0] % 1000).astype(jnp.float32) * jnp.float32(2.0 * math.pi / 1000.0)
    return jnp.float32(0.25) * (jnp.float32(0.55) + jnp.float32(0.45) * jnp.cos(phase))


def across(rows, lanes=128):
    n = rows.shape[1]
    return jnp.broadcast_to(rows[None], (lanes // 8, 8, n)).reshape(lanes, n).T


def kernel(
    level, nz, early,
    gate, up, target, gain, weight, rate,
    normed, mixed,
    gate_v, up_v, target_v, w_v, h_v, ht_v, p_v, mx_v, left_v, right_v, own_v,
    ql_v, qr_v, q2_v, qs_v, rl_v, rr_v, r2_v, rs_v, tr_v, st_v, rst_v,
    norm_v, grad_v, their_grad_v, their_ht_v, upd_v, peer_v, relay_v,
    in_sem, w_sem, out_sem, mix_sem, qss, qrs, q2s, q2r, sss, srs, tss, trs, bss, brs, css, crs, fss, frs, ess, ers,
):
    share = target_v.shape[1]
    ff = w_v.shape[1]
    chunk = h_v.shape[1]
    z, xl, c, y, xh = (lax.axis_index(a) for a in ("z", "xl", "c", "y", "xh"))
    mine = y * 2 + xh

    def offset(k):
        j = lax.div(k, 2)
        return lax.rem(lax.div(j * (j + 1), 2), 4), lax.rem(k, 2)

    def member(k):
        dy, dx = offset(k)
        return lax.rem(y + dy, N_Y), lax.rem(xh + dx, 2)

    def device(k):
        py, px = member(k)
        return {"y": py, "xh": px}

    def owner(k):
        py, px = member(k)
        return py * 2 + px

    def seen_as(k):
        j = lax.div(k, 2)
        return (2 * j - 3 * lax.div(j, 2)) * 2 + lax.rem(k, 2)

    def gossip(by):
        to = lax.rem(z * 4 + xl * 2 + c + by, nz * 4)
        return {"z": lax.div(to, 4), "xl": lax.rem(lax.div(to, 2), 2), "c": lax.rem(to, 2)}

    target_device = gossip(1 << level)
    source_device = gossip(nz * 4 - (1 << level))
    diagonal = level < 2
    around = RELAYED if level == 3 and nz == 8 else 0
    if diagonal:
        sends_far = jnp.logical_and(xl == 1, c == 1) if level == 0 else xl == 1
        relays = jnp.logical_and(xl == 0, c == 0) if level == 0 else xl == 0
        relay_count = (1 - xl) * (1 - c) if level == 0 else 1 - xl
        onward = {"z": lax.rem(z + 1, nz)}
        behind = {"z": lax.rem(z + nz - 1, nz)}
        side = {"xl": 1 - xl, "c": 1 - c} if level == 0 else {"xl": 1 - xl}
    elif around:
        onward = {"z": lax.rem(z + nz - 3, nz)}
        behind = {"z": lax.rem(z + 3, nz)}

    def load(i, which):
        src, dst = ((gate, gate_v), (up, up_v))[which]
        return pltpu.make_async_copy(src.at[pl.ds(i * chunk, chunk)], dst.at[i], in_sem.at[which, i])

    def load_w(k):
        return pltpu.make_async_copy(weight.at[:, pl.ds(k * share, share)], w_v.at[k], w_sem.at[k])

    target_load = pltpu.make_async_copy(target, target_v, in_sem.at[2, 0])
    for which in range(2):
        load(0, which).start()
    for k in range(N_TP):
        load_w(k).start()
    for i in range(1, N_CHUNKS):
        for which in range(2):
            load(i, which).start()
    target_load.start()

    barrier = pltpu.get_barrier_semaphore()
    for k in range(1, N_TP):
        pl.semaphore_signal(barrier, inc=1, device_id=device(jnp.int32(k)), device_id_type=MESH)
    if diagonal:

        @pl.when(relays)
        def _():
            pl.semaphore_signal(barrier, inc=1, device_id=side, device_id_type=MESH)
            pl.semaphore_signal(barrier, inc=1, device_id=behind, device_id_type=MESH)

        @pl.when(jnp.logical_not(relays))
        def _():
            pl.semaphore_signal(barrier, inc=1, device_id=source_device, device_id_type=MESH)

    else:
        pl.semaphore_signal(barrier, inc=1, device_id=source_device, device_id_type=MESH)
        if around:
            pl.semaphore_signal(barrier, inc=1, device_id=behind, device_id_type=MESH)

    half = share // 2

    def peer(d):
        return {"y": lax.rem(y + d, N_Y)} if d else {"xh": 1 - xh}

    def first_copy(i, d):
        s = (N_Y - d) % N_Y
        return pltpu.make_async_remote_copy(
            src_ref=ql_v.at[i, d - 1] if d else qr_v.at[i], dst_ref=rl_v.at[i, s - 1] if d else rr_v.at[i],
            send_sem=qss.at[i, d], recv_sem=qrs.at[i, s], device_id=peer(d), device_id_type=MESH,
        )

    def second_copy(i, d):
        s = (N_Y - d) % N_Y
        return pltpu.make_async_remote_copy(
            src_ref=q2_v.at[i, d], dst_ref=r2_v.at[i, s], send_sem=q2s.at[i, d], recv_sem=q2r.at[i, s],
            device_id=peer(d), device_id_type=MESH,
        )

    def scale_copy(stage, i, d):
        s = (N_Y - d) % N_Y
        return pltpu.make_async_remote_copy(
            src_ref=qs_v.at[stage, i], dst_ref=rs_v.at[stage, i, s],
            send_sem=sss.at[stage, i, d], recv_sem=srs.at[stage, i, s],
            device_id=peer(d), device_id_type=MESH,
        )

    def coded(values):
        return jnp.round(values).astype(jnp.int32).astype(jnp.int16)

    def decoded(codes):
        return codes.astype(jnp.int32).astype(jnp.float32)

    def send_stage(stage, i):
        for d in range(N_Y):
            scale_copy(stage, i, d).start()
            (first_copy, second_copy)[stage](i, d).start()

    def receive_stage(stage, i):
        for d in range(N_Y):
            scale_copy(stage, i, d).wait_recv()
            (first_copy, second_copy)[stage](i, d).wait_recv()
        scales = jnp.zeros((8, chunk), jnp.float32)
        for d in range(N_Y):
            scales = jnp.where(sub == d, rs_v[stage, i, d], scales)
        tr_v[...] = across(scales)

    sub = lax.broadcasted_iota(jnp.int32, (8, chunk), 0)
    lane = lax.broadcasted_iota(jnp.int32, (ROWS, 128), 1)

    def early_copy(n):
        rows = pl.ds(0, early)
        src, dst = (
            (w_v.at[:, rows], peer_v.at[:, rows]),
            (ht_v.at[rows], their_ht_v),
            (grad_v.at[mine], their_grad_v.at[mine]),
        )[n]
        return pltpu.make_async_remote_copy(
            src_ref=src, dst_ref=dst, send_sem=ess.at[n], recv_sem=ers.at[n],
            device_id=target_device, device_id_type=MESH,
        )

    def project(i, _):
        load(i, 0).wait()
        load(i, 1).wait()

        def hidden_rows(r, _):
            rows = pl.ds(r * ROWS, ROWS)
            v = gate_v[i, rows, :].astype(jnp.float32)
            h = v / (1.0 + jnp.exp(-v)) * up_v[i, rows, :].astype(jnp.float32)
            h_v[i, rows, :] = h.astype(jnp.bfloat16)
            return 0

        lax.fori_loop(0, chunk // ROWS, hidden_rows, 0)

        @pl.when(i == 0)
        def _():
            for k in range(N_TP):
                load_w(k).wait()
            pl.semaphore_wait(barrier, N_TP + (relay_count if diagonal else 1 if around else 0))
            if early:
                early_copy(0).start()

        mx_v[...] = jnp.zeros_like(mx_v)

        def product(k, _):
            part = jnp.dot(h_v[i], w_v[k], preferred_element_type=jnp.float32)
            p_v[k] = part
            size = jnp.abs(part)
            for half in range(share // 128):
                mx_v[...] = jnp.maximum(mx_v[...], size[:, half * 128 : (half + 1) * 128])
            return 0

        lax.fori_loop(0, N_TP, product, 0)
        largest = jnp.maximum(jnp.max(mx_v[...], axis=1, keepdims=True), 1e-30)
        mx_v[...] = jnp.broadcast_to(CODE_MAX / largest, mx_v.shape)
        qs_v[0, i] = jnp.broadcast_to(largest * (1.0 / CODE_MAX), mx_v.shape).T[0:8, :]

        def code_rows(r, _):
            rows = pl.ds(r * ROWS, ROWS)
            inverse = mx_v[rows, :]
            for h in range(2):
                left_v[i, h, rows, :] = p_v[y * 2 + h, rows, :half]
                for d in range(1, N_Y):
                    ql_v[i, d - 1, h, rows, :] = coded(p_v[lax.rem(y + d, N_Y) * 2 + h, rows, :half] * inverse)
            for n in range(N_Y):
                right_v[i, n, rows, :] = p_v[n * 2 + xh, rows, half:]
                qr_v[i, n, rows, :] = coded(p_v[n * 2 + 1 - xh, rows, half:] * inverse)
            return 0

        lax.fori_loop(0, chunk // ROWS, code_rows, 0)
        send_stage(0, i)
        return 0

    lax.fori_loop(0, N_CHUNKS, project, 0)

    for i in range(N_CHUNKS):
        ht_v[:, i * chunk : (i + 1) * chunk] = h_v[i].T
    if early:
        early_copy(1).start()

    def combine(i, _):
        receive_stage(0, i)

        def combine_rows(r, _):
            rows = pl.ds(r * ROWS, ROWS)
            scale = tr_v[rows, :]
            for h in range(2):
                total = left_v[i, h, rows, :]
                for s in range(1, N_Y):
                    total = total + decoded(rl_v[i, s - 1, h, rows, :]) * scale[:, s : s + 1]
                left_v[i, h, rows, :] = total
            for n in range(N_Y):
                right_v[i, n, rows, :] = right_v[i, n, rows, :] + decoded(rr_v[i, n, rows, :]) * scale[:, 0:1]
            parts = [left_v[i, 1 - xh, rows, :]]
            parts += [right_v[i, lax.rem(y + d, N_Y), rows, :] for d in range(1, N_Y)]
            size = functools.reduce(jnp.maximum, [jnp.abs(part) for part in parts])
            largest = jnp.maximum(jnp.max(size, axis=1, keepdims=True), 1e-30)
            inverse = CODE_MAX / largest
            for d in range(N_Y):
                q2_v[i, d, rows, :] = coded(parts[d] * inverse)
            mx_v[rows, :] = jnp.broadcast_to(largest * (1.0 / CODE_MAX), (ROWS, 128))
            return 0

        lax.fori_loop(0, chunk // ROWS, combine_rows, 0)
        qs_v[1, i] = mx_v[...].T[0:8, :]
        send_stage(1, i)
        return 0

    lax.fori_loop(0, N_CHUNKS, combine, 0)

    def stat_copy(i, k):
        s = seen_as(k)
        return pltpu.make_async_remote_copy(
            src_ref=st_v.at[i], dst_ref=rst_v.at[i, s], send_sem=tss.at[i, k], recv_sem=trs.at[i, s],
            device_id=device(k), device_id_type=MESH,
        )

    target_load.wait()

    def reduce(i, _):
        receive_stage(1, i)

        def reduce_rows(r, _):
            rows = pl.ds(r * ROWS, ROWS)
            scale = tr_v[rows, :]
            left = left_v[i, xh, rows, :] + decoded(r2_v[i, 0, rows, :]) * scale[:, 0:1]
            right = right_v[i, y, rows, :]
            for d in range(1, N_Y):
                right = right + decoded(r2_v[i, d, rows, :]) * scale[:, d : d + 1]
            total = jnp.concatenate([left, right], axis=1)
            s = total * FF ** (-0.5)
            own_v[i, rows, :] = s
            g = gain[...]
            t = target_v[pl.ds(i * chunk + r * ROWS, ROWS), :].astype(jnp.float32)
            gs = g * s
            a = jnp.sum(s * s, axis=1, keepdims=True)
            b = jnp.sum(gs * gs, axis=1, keepdims=True)
            d = jnp.sum(gs * t, axis=1, keepdims=True)
            tr_v[rows, :] = jnp.where(lane == 0, a, jnp.where(lane == 1, b, d))
            return 0

        lax.fori_loop(0, chunk // ROWS, reduce_rows, 0)
        st_v[i] = tr_v[...].T[0:8, :]

        def send(k, _):
            stat_copy(i, k).start()
            return 0

        lax.fori_loop(1, N_TP, send, 0)
        return 0

    lax.fori_loop(0, N_CHUNKS, reduce, 0)

    width = share * N_TP

    def finish(i, _):
        sums = st_v[i]
        for k in range(1, N_TP):
            stat_copy(i, jnp.int32(k)).wait_recv()
        for k in range(1, N_TP):
            sums = sums + rst_v[i, k]
        tr_v[...] = across(sums)

        def finish_rows(r, _):
            rows = pl.ds(r * ROWS, ROWS)
            at = pl.ds(i * chunk + r * ROWS, ROWS)
            sums = tr_v[rows, :] * (1.0 / width)
            inv = lax.rsqrt(sums[:, 0:1] + EPSILON)
            inner = inv * inv * sums[:, 1:2] - inv * sums[:, 2:3]
            g = gain[...]
            normal = own_v[i, rows, :] * inv
            output = normal * g
            grad_norm = (output - target_v[at, :].astype(jnp.float32)) * g
            norm_v[at, :] = output.astype(jnp.bfloat16)
            grad_v[mine, at, :] = (inv * (grad_norm - normal * inner)).astype(jnp.bfloat16)
            return 0

        lax.fori_loop(0, chunk // ROWS, finish_rows, 0)
        return 0

    lax.fori_loop(0, N_CHUNKS, finish, 0)

    token_half = grad_v.shape[1] // 2

    def share_copy(b, which, k):
        buf = (grad_v, their_grad_v)[b]
        at = owner(jnp.int32(which))
        return pltpu.make_async_remote_copy(
            src_ref=buf.at[at], dst_ref=buf.at[at], send_sem=bss.at[b, k + which], recv_sem=brs.at[b, seen_as(k) + which],
            device_id=device(k), device_id_type=MESH,
        )

    def passed_on(b, k):
        buf = (grad_v, their_grad_v)[b]
        j = lax.div(k, 2)
        h = 2 - j
        part = buf.at[owner(k), pl.ds(pl.multiple_of(h * token_half, token_half), token_half)]
        sem = N_TP - 2 + lax.rem(k, 2) + 2 * h
        return pltpu.make_async_remote_copy(
            src_ref=part, dst_ref=part, send_sem=bss.at[b, sem], recv_sem=brs.at[b, sem],
            device_id={"y": lax.rem(y + N_Y + 1 - 2 * j, N_Y)}, device_id_type=MESH,
        )

    def near_arrival(b, k):
        buf = (grad_v, their_grad_v)[b]
        at = owner(k)
        return pltpu.make_async_remote_copy(
            src_ref=buf.at[at], dst_ref=buf.at[at], send_sem=bss.at[b, k], recv_sem=brs.at[b, k],
            device_id=device(k), device_id_type=MESH,
        )

    def far_arrival(b, k, h):
        buf = (grad_v, their_grad_v)[b]
        part = buf.at[owner(k), pl.ds(h * token_half, token_half)]
        return pltpu.make_async_remote_copy(
            src_ref=part, dst_ref=part, send_sem=bss.at[b, k + 2 * h], recv_sem=brs.at[b, k + 2 * h],
            device_id=device(k), device_id_type=MESH,
        )

    def send_own(b):
        for k in (1, 2, 4):
            share_copy(b, 0, jnp.int32(k)).start()

    def receive_near(b, k):
        near_arrival(b, k).wait_recv()

        @pl.when(k == 1)
        def _():
            for j in (2, 4):
                share_copy(b, 1, jnp.int32(j)).start()

        @pl.when(k > 1)
        def _():
            passed_on(b, k).start()

    def receive_far(b, k):
        for h in range(2):
            far_arrival(b, k, h).wait_recv()

    send_own(0)
    if early:
        early_copy(2).start()
    normed_out = pltpu.make_async_copy(norm_v, normed, out_sem.at[0])
    normed_out.start()

    pieces = PIECES if level == 1 else 1
    length = (ff - early) // pieces

    def late(p):
        return pl.ds(early + p * length, length)

    def gossip_copy(k, p):
        at, n = owner(k), k * pieces + p
        return pltpu.make_async_remote_copy(
            src_ref=upd_v.at[at, late(p)], dst_ref=peer_v.at[at, late(p)], send_sem=css.at[n], recv_sem=crs.at[n],
            device_id=target_device, device_id_type=MESH,
        )

    def first_leg(k, p):
        at, n = owner(k), k * pieces + p
        return pltpu.make_async_remote_copy(
            src_ref=upd_v.at[at, late(p)], dst_ref=relay_v.at[k, pl.ds(p * length, length)],
            send_sem=css.at[n], recv_sem=frs.at[n],
            device_id=side if diagonal else onward, device_id_type=MESH,
        )

    def second_leg(k, p):
        at, n = owner(k), k * pieces + p
        return pltpu.make_async_remote_copy(
            src_ref=relay_v.at[k, pl.ds(p * length, length)], dst_ref=peer_v.at[at, late(p)],
            send_sem=fss.at[n], recv_sem=crs.at[n],
            device_id=onward, device_id_type=MESH,
        )

    def forward(k):
        for p in range(pieces):
            first_leg(k, p).wait_recv()
            second_leg(k, p).start()

    def send_updated(k):
        if diagonal:

            @pl.when(sends_far)
            def _():
                for p in range(pieces):
                    first_leg(k, p).start()

            @pl.when(jnp.logical_not(sends_far))
            def _():
                for p in range(pieces):
                    gossip_copy(k, p).start()

            @pl.when(jnp.logical_and(relays, k >= LAG))
            def _():
                forward(k - LAG)

        elif around:

            @pl.when(k < around)
            def _():
                first_leg(k, 0).start()

            @pl.when(k >= around)
            def _():
                gossip_copy(k, 0).start()

        else:
            gossip_copy(k, 0).start()

    step = rate[0]

    def update(k, _):
        at = owner(k)

        @pl.when(jnp.logical_and(k > 0, k < N_TP - 2))
        def _():
            receive_near(0, k)

        @pl.when(k >= N_TP - 2)
        def _():
            receive_far(0, k)

        weight_grad = jnp.dot(ht_v[...], grad_v[at], preferred_element_type=jnp.float32) * FF ** (-0.5)
        upd_v[at] = (w_v[at].astype(jnp.float32) - step * weight_grad).astype(jnp.bfloat16)
        send_updated(k)
        return 0

    lax.fori_loop(0, N_TP, update, 0)
    if diagonal:

        @pl.when(relays)
        def _():
            for k in range(N_TP - LAG, N_TP):
                forward(jnp.int32(k))

    if early:
        early_copy(2).wait_recv()
        send_own(1)

        def pass_theirs(k, _):
            receive_near(1, k)
            return 0

        lax.fori_loop(1, N_TP - 2, pass_theirs, 0)
        early_copy(0).wait()
        early_copy(1).wait()
    for k in range(around):
        forward(jnp.int32(k))

    def mixed_out(k):
        at = owner(k)
        return pltpu.make_async_copy(
            w_v.at[at], mixed.at[:, pl.ds(pl.multiple_of(at * share, share), share)], mix_sem.at[k]
        )

    def average(number, _):
        k = lax.rem(number + around, N_TP)
        at = owner(k)
        if early:

            @pl.when(k >= N_TP - 2)
            def _():
                receive_far(1, k)

            weight_grad = jnp.dot(their_ht_v[...], their_grad_v[at], preferred_element_type=jnp.float32) * FF ** (-0.5)
            theirs = peer_v[at, :early, :].astype(jnp.float32) - step * weight_grad
            peer_v[at, :early, :] = theirs.astype(jnp.bfloat16)
        for p in range(pieces):
            gossip_copy(k, p).wait_recv()

        def average_rows(r, _):
            rows = pl.ds(r * ROWS, ROWS)
            both = upd_v[at, rows, :].astype(jnp.float32) + peer_v[at, rows, :].astype(jnp.float32)
            w_v[at, rows, :] = (0.5 * both).astype(jnp.bfloat16)
            return 0

        lax.fori_loop(0, ff // ROWS, average_rows, 0)
        mixed_out(k).start()
        return 0

    lax.fori_loop(0, N_TP, average, 0)

    def drain(k, _):
        def drain_chunk(i, _):
            stat_copy(i, k).wait_send()
            return 0

        lax.fori_loop(0, N_CHUNKS, drain_chunk, 0)
        return 0

    lax.fori_loop(1, N_TP, drain, 0)

    def drain_shares(k, _):
        for b in range(2 if early else 1):
            near_arrival(b, k).wait_send()
        return 0

    lax.fori_loop(1, N_TP - 2, drain_shares, 0)
    for k in (N_TP - 2, N_TP - 1):
        for h in range(2):
            for b in range(2 if early else 1):
                far_arrival(b, jnp.int32(k), h).wait_send()
    if early:
        early_copy(2).wait_send()

    def drain_stages(i, _):
        for d in range(N_Y):
            first_copy(i, d).wait_send()
            second_copy(i, d).wait_send()
            for stage in range(2):
                scale_copy(stage, i, d).wait_send()
        return 0

    lax.fori_loop(0, N_CHUNKS, drain_stages, 0)

    def drain_mixed(k, _):
        for p in range(pieces):
            gossip_copy(k, p).wait_send()
        if diagonal:

            @pl.when(relays)
            def _():
                for p in range(pieces):
                    second_leg(k, p).wait_send()
        mixed_out(k).wait()
        return 0

    lax.fori_loop(0, N_TP, drain_mixed, 0)
    for k in range(around):
        second_leg(jnp.int32(k), 0).wait_send()
    normed_out.wait()


def step_at(level, nz, gate, up, target, gain, weight, rate):
    tok, ff = gate.shape
    share = target.shape[1]
    chunk = tok // N_CHUNKS
    early = EARLY.get(level, 0) if (nz, ff) == (8, 896) else 0
    bf16, f32, i16 = jnp.bfloat16, jnp.float32, jnp.int16
    dma = pltpu.SemaphoreType.DMA
    hbm = pl.BlockSpec(memory_space=pl.ANY)
    return pl.pallas_call(
        functools.partial(kernel, level, nz, early),
        out_shape=(
            jax.ShapeDtypeStruct((tok, share), bf16),
            jax.ShapeDtypeStruct(weight.shape, bf16),
        ),
        in_specs=[hbm, hbm, hbm, pl.BlockSpec(memory_space=pltpu.VMEM), hbm, pl.BlockSpec(memory_space=pltpu.SMEM)],
        out_specs=(hbm, hbm),
        scratch_shapes=[
            pltpu.VMEM((N_CHUNKS, chunk, ff), bf16),
            pltpu.VMEM((N_CHUNKS, chunk, ff), bf16),
            pltpu.VMEM((tok, share), bf16),
            pltpu.VMEM((N_TP, ff, share), bf16),
            pltpu.VMEM((N_CHUNKS, chunk, ff), bf16),
            pltpu.VMEM((ff, tok), bf16),
            pltpu.VMEM((N_TP, chunk, share), f32),
            pltpu.VMEM((chunk, 128), f32),
            pltpu.VMEM((N_CHUNKS, 2, chunk, share // 2), f32),
            pltpu.VMEM((N_CHUNKS, N_Y, chunk, share // 2), f32),
            pltpu.VMEM((N_CHUNKS, chunk, share), f32),
            pltpu.VMEM((N_CHUNKS, N_Y - 1, 2, chunk, share // 2), i16),
            pltpu.VMEM((N_CHUNKS, N_Y, chunk, share // 2), i16),
            pltpu.VMEM((N_CHUNKS, N_Y, chunk, share // 2), i16),
            pltpu.VMEM((2, N_CHUNKS, 8, chunk), f32),
            pltpu.VMEM((N_CHUNKS, N_Y - 1, 2, chunk, share // 2), i16),
            pltpu.VMEM((N_CHUNKS, N_Y, chunk, share // 2), i16),
            pltpu.VMEM((N_CHUNKS, N_Y, chunk, share // 2), i16),
            pltpu.VMEM((2, N_CHUNKS, N_Y, 8, chunk), f32),
            pltpu.VMEM((chunk, 128), f32),
            pltpu.VMEM((N_CHUNKS, 8, chunk), f32),
            pltpu.VMEM((N_CHUNKS, N_TP, 8, chunk), f32),
            pltpu.VMEM((tok, share), bf16),
            pltpu.VMEM((N_TP, tok, share), bf16),
            pltpu.VMEM((N_TP, tok if early else 16, share), bf16),
            pltpu.VMEM((max(early, 16), tok), bf16),
            pltpu.VMEM((N_TP, ff, share), bf16),
            pltpu.VMEM((N_TP, ff, share), bf16),
            pltpu.VMEM((N_TP if level < 2 else RELAYED, ff - early, share), bf16),
            dma((3, N_CHUNKS)),
            dma((N_TP,)),
            dma((1,)),
            dma((N_TP,)),
            dma((N_CHUNKS, N_Y)),
            dma((N_CHUNKS, N_Y)),
            dma((N_CHUNKS, N_Y)),
            dma((N_CHUNKS, N_Y)),
            dma((2, N_CHUNKS, N_Y)),
            dma((2, N_CHUNKS, N_Y)),
            dma((N_CHUNKS, N_TP)),
            dma((N_CHUNKS, N_TP)),
            dma((2, N_TP + 2)),
            dma((2, N_TP + 2)),
            dma((N_TP * PIECES,)),
            dma((N_TP * PIECES,)),
            dma((N_TP * PIECES,)),
            dma((N_TP * PIECES,)),
            dma((3,)),
            dma((3,)),
        ],
        compiler_params=pltpu.CompilerParams(
            collective_id=level + 1, has_side_effects=True, vmem_limit_bytes=56 << 20
        ),
        name=f"step_level{level}",
    )(gate, up, target, gain, weight, rate)


def shards(nz, gate_pre, up_pre, target, norm_gain, weight, round_index):
    levels = (nz * 4).bit_length() - 1
    rate = step_rate(round_index).reshape(1)
    level = round_index[0] % levels
    operands = (gate_pre, up_pre, target, norm_gain.reshape(1, -1), weight[0], rate)
    branches = [functools.partial(step_at, number, nz) for number in range(levels)]
    normed, mixed = lax.switch(level, branches, *operands)
    return (normed, mixed[None])


def solution(mesh):
    nz = mesh.shape["dp"] // 4
    axes = ("z", "xl", "c", "y", "xh")
    finer = Mesh(mesh.devices.reshape(nz, 2, 2, N_Y, 2), axes)
    dp, tp = axes[:3], axes[3:]
    return jax.shard_map(
        functools.partial(shards, nz),
        mesh=finer,
        in_specs=(P(dp, tp), P(dp, tp), P(dp, tp), P(tp), P(dp, tp, None), P()),
        out_specs=(P(dp, tp), P(dp, tp, None)),
        check_vma=False,
    )
```
